32 devices in a mesh: dp: 16 (over z, x, core), tensor: 2 (over y).
Axes of the slice: x: 2, y: 2, z: 4, core: 2. Of those that a mesh axis runs over, the one named last changes fastest.
Arguments:
- hidden: bfloat16 [5120, 18432], P('dp', 'tensor'), may hold values from -6 to 6
- fixed_down_weight: bfloat16 [18432, 4608], P('tensor', 'dp'), may hold values from -4 to 4
- lowrank_factor_b: bfloat16 [18432, 16], P('tensor'), may hold values from -0.046875 to 0.046875
- lowrank_factor_a: bfloat16 [16, 4608], P(None, 'dp'), may hold values from -1.5 to 1.5
- magnitude: float32 [4608], P('tensor'), may hold values from 0.5 to 2
- cotangent: bfloat16 [5120, 4608], P('dp', 'tensor'), may hold values from -0.083496094 to 0.083496094
Outputs:
- mixed: bfloat16 [5120, 4608], P('dp', 'tensor')
- gradient_column_scale: float32 [4608], P(('tensor', 'dp'))
- gradient_factor_a: float32 [16, 4608], P(None, ('tensor', 'dp'))
- gradient_factor_b: float32 [18432, 16], P(('tensor', 'dp'))
The draws below stay inside these ranges and needn't reach their ends.
All inputs are finite; a program needn't handle non-finite values.
Results may differ from the reference program's by a relative error of at most 0.0054.
Values may be sent and summed in bfloat16 or wider, within the bound.
A program may use at most 192 MiB of HBM per device.

```python
import math
import jax
import jax.numpy as jnp
from jax import lax

MODEL_WIDTH = 4608
HALF_FEEDFORWARD = 18432
ADAPTER_RANK = 16
TOK_DEV = 320
TOKENS = 5120
N_DP = 16


def draw_fixed_down_weight(key, part):
    base = jax.random.truncated_normal(key, -4.0, 4.0, (HALF_FEEDFORWARD, MODEL_WIDTH), jnp.float32) * HALF_FEEDFORWARD ** (-0.5)
    ramp = 0.5 + jnp.arange(HALF_FEEDFORWARD, dtype=jnp.float32) / (HALF_FEEDFORWARD - 1)
    return (base * ramp[:, None]).astype(jnp.bfloat16)


def raised(array, rng, source, target, shards_of, factor):
    owner, partner = [(jnp.arange(array.shape[dim]) // (array.shape[dim] // shards_of)).reshape([-1 if axis == dim else 1 for axis in range(array.ndim)]) for dim in (source, target)]
    chosen = jax.random.permutation(rng, shards_of)[partner]
    strong = (owner == chosen) | (owner == (partner + shards_of // 2) % shards_of)
    return jnp.where(strong, factor * array, array)


def levels(key, extent, shards, low, largest):
    factor_of = 1.0
    for axis_at, shards_of in shards:
        steps = jax.random.uniform(jax.random.fold_in(jax.random.fold_in(key, 6), axis_at), (shards_of,), jnp.float32, low / len(shards), largest / len(shards))
        factor_of = factor_of * jnp.repeat(jnp.exp(steps), extent[axis_at] // shards_of).reshape((-1,) + (1,) * (len(extent) - 1 - axis_at))
    return factor_of


def normal_values(rng, extent, deviation, limit, pieces=(), held_as=jnp.bfloat16):
    gain = levels(rng, extent, pieces, -0.22, 0.18) if pieces else 1.0
    values = jax.random.normal(rng, extent, jnp.float32) * deviation * gain
    return jnp.minimum(jnp.maximum(values, -limit), limit).astype(held_as)


def bell_draw_with(own_key, extent, spread, bound, cuts, heavy, held_as=jnp.bfloat16):
    array = spread * jax.random.normal(own_key, extent, jnp.float32)
    if cuts:
        array = array * levels(own_key, extent, cuts, -0.22, 0.18)
    return jnp.clip(raised(array, jax.random.fold_in(own_key, 3), *heavy), -bound, bound).astype(held_as)


def setup_inputs(seed: int = 0) -> dict:
    arg_keys = jax.random.split(jax.random.key(seed), 7)
    return {
        "hidden": bell_draw_with(arg_keys[0], (TOKENS, HALF_FEEDFORWARD), 1.0, 6.0, ((0, 16), (1, 2)), (0, 1, 16, 2.0)),
        "fixed_down_weight": draw_fixed_down_weight(jax.random.fold_in(arg_keys[6], 71), 0),
        "lowrank_factor_b": normal_values(arg_keys[2], (HALF_FEEDFORWARD, ADAPTER_RANK), HALF_FEEDFORWARD ** -0.5, 0.046875, ((0, 2),)),
        "lowrank_factor_a": normal_values(arg_keys[3], (ADAPTER_RANK, MODEL_WIDTH), ADAPTER_RANK ** -0.5, 1.5, ((1, 16),)),
        "magnitude": jnp.clip(jnp.exp(math.log(2.0) - 1.3862944 * jax.random.uniform(arg_keys[4], (MODEL_WIDTH,), jnp.float32) ** levels(arg_keys[4], (MODEL_WIDTH,), ((0, 2),), -0.2, 0.2)), 0.5, 2.0),
        "cotangent": bell_draw_with(arg_keys[5], (TOKENS, MODEL_WIDTH), ((TOK_DEV * N_DP) ** -0.5), 0.083496094, ((0, 16), (1, 2)), (0, 1, 16, 2.0)),
    }


def squared_column_entries(fixed_down_weight, lowrank_factor_b, lowrank_factor_a):
    w_blocks = fixed_down_weight.reshape(8, HALF_FEEDFORWARD // 8, MODEL_WIDTH)
    factor_b_blocks = lowrank_factor_b.reshape(8, HALF_FEEDFORWARD // 8, ADAPTER_RANK)

    def one_block(pair):
        weight_tile_block, factor_b_block = pair
        combined_weight = weight_tile_block.astype(jnp.float32) + jnp.dot(factor_b_block, lowrank_factor_a, preferred_element_type=jnp.float32)
        return lax.optimization_barrier(jnp.sum(combined_weight * combined_weight, axis=0))
    return lax.optimization_barrier(jnp.sum(lax.map(one_block, (w_blocks, factor_b_blocks)), axis=0))

def reference(hidden, fixed_down_weight, lowrank_factor_b, lowrank_factor_a, magnitude, cotangent):
    column_norm_values = jnp.sqrt(squared_column_entries(fixed_down_weight, lowrank_factor_b, lowrank_factor_a) + 1e-06)
    scale = magnitude / column_norm_values
    lowrank_update = jnp.dot(hidden, lowrank_factor_b, preferred_element_type=jnp.float32)
    lowrank_block_update = lowrank_update.astype(jnp.bfloat16)
    prenorm_output = jnp.dot(hidden, fixed_down_weight, preferred_element_type=jnp.float32) + jnp.dot(lowrank_block_update, lowrank_factor_a, preferred_element_type=jnp.float32)
    mixed = (prenorm_output * scale).astype(jnp.bfloat16)
    cot = cotangent.astype(jnp.float32)
    gradient_column_scale = lax.optimization_barrier(jnp.sum(cot * prenorm_output, axis=0)) / column_norm_values
    prenorm_gradient_b = (cot * scale).astype(jnp.bfloat16)
    gradient_factor_a = jnp.dot(lowrank_block_update.T, prenorm_gradient_b, preferred_element_type=jnp.float32)
    backward_factor_b = jnp.dot(prenorm_gradient_b, lowrank_factor_a.T, preferred_element_type=jnp.float32).astype(jnp.bfloat16)
    gradient_factor_b = jnp.dot(hidden.T, backward_factor_b, preferred_element_type=jnp.float32)
    return (mixed, gradient_column_scale, gradient_factor_a, gradient_factor_b)
```

```python
import functools

import jax
import jax.numpy as jnp
from jax import lax
from jax.experimental import pallas as pl
from jax.experimental.pallas import tpu as pltpu
from jax.sharding import Mesh, PartitionSpec as P

F32, BF16 = jnp.float32, jnp.bfloat16
AXES = ("u", "b", "x", "core", "tensor")
NT = (((1,), (1,)), ((), ()))
N_CHUNK = 3
H_CHUNK = 4


def split_of(size, most):
    best = 128
    for step in range(128, most + 1, 128):
        if size % step == 0:
            best = step
    return best


def bulk_kernel(
    n_u, n_x, h, w, out, hs, ws, own, part_out, part_in, scat,
    loc_sem, hc_sem, hb_sem, hr_sem, wx_sem, wa_sem, wr_sem, ps_sem, pr_sem, ss_sem, sr_sem,
):
    u, b, x, c, t = (lax.axis_index(a) for a in AXES)
    rows, depth = h.shape
    cols = w.shape[0]
    cw = cols // N_CHUNK
    hr = rows // H_CHUNK
    kc = split_of(depth, 1152)

    def at(**moved):
        here = dict(u=u, b=b, x=x, core=c, tensor=t)
        here.update(moved)
        return tuple(here[a] for a in AXES)

    def shift(value, by, n):
        return lax.rem(value + by, n)

    def far_b(k):
        return shift(b, k % 2, 2)

    core_peer = at(core=1 - c)
    b_peer = at(b=1 - b)
    diag_peer = at(b=1 - b, core=1 - c)
    x_to = [at(x=shift(x, k, n_x)) for k in range(n_x)]
    u_to = [at(u=shift(u, k, n_u), b=far_b(k)) for k in range(n_u)]
    t_to = [at(tensor=shift(t, k, n_u)) for k in range(n_u)]

    peers = [core_peer, b_peer, diag_peer] + x_to[1:] + u_to[1:] + t_to[1:]
    barrier = pltpu.get_barrier_semaphore()
    for peer in peers:
        pl.semaphore_signal(barrier, inc=1, device_id=peer, device_id_type=pl.DeviceIdType.MESH)
    pl.semaphore_wait(barrier, len(peers))

    def send(src, dst, sems, index, peer):
        return pltpu.make_async_remote_copy(
            src_ref=src,
            dst_ref=dst,
            send_sem=sems.at[(0,) + index],
            recv_sem=sems.at[(1,) + index],
            device_id=peer,
            device_id_type=pl.DeviceIdType.MESH,
        )

    def h_rows(bb, cc, i):
        return hs.at[bb, pl.ds(pl.multiple_of(cc * rows + i * hr, 16), hr), :]

    def w_rows(uu, xx, j):
        return ws.at[uu, xx, pl.ds(j * cw, cw), :]

    own_rows = hs.at[b, pl.ds(pl.multiple_of(c * rows, 16), rows), :]
    sent = []

    loads = [
        pltpu.make_async_copy(h, own_rows, loc_sem.at[0]),
        pltpu.make_async_copy(w, ws.at[u, x], loc_sem.at[1]),
    ]
    for load in loads:
        load.start()
    h_core = send(h, own_rows, hc_sem, (0,), core_peer)
    h_core.start()
    for i in range(H_CHUNK):
        copy = send(h.at[pl.ds(i * hr, hr), :], h_rows(b, c, i), hb_sem, (i,), b_peer)
        copy.start()
        sent.append(copy)
    for j in range(N_CHUNK):
        piece = w.at[pl.ds(j * cw, cw), :]
        for k in range(1, n_x):
            copy = send(piece, w_rows(u, x, j), wx_sem, (k - 1, j), x_to[k])
            copy.start()
            sent.append(copy)
        for k in range(1, n_u):
            copy = send(piece, w_rows(u, x, j), wa_sem, (k - 1, j), u_to[k])
            copy.start()
            sent.append(copy)

    def unit(bb, uu, j, take):
        def step(i, acc):
            at_k = pl.ds(pl.multiple_of(i * kc, 128), kc)
            left = hs[bb, :, at_k]
            right = jnp.concatenate([ws[uu, xx, j * cw : (j + 1) * cw, at_k] for xx in range(n_x)], axis=0)
            return acc + lax.dot_general(left, right, NT, preferred_element_type=F32)

        zero = jnp.zeros((2 * rows, n_x * cw), F32)
        take(lax.fori_loop(0, depth // kc, step, zero))

    count = [0]
    waiting = [[], []]

    def run_unit(kb, ku, j):
        place = count[0] % 2
        count[0] += 1
        bb, uu = shift(b, kb, 2), shift(u, ku, n_u)
        keep = uu == t
        slot = kb * N_CHUNK + j

        def copy():
            return send_part(slot, place, uu)

        if waiting[place]:
            old_keep, old_copy = waiting[place].pop()

            @pl.when(jnp.logical_not(old_keep))
            def _():
                old_copy().wait_send()

        def take(value):
            @pl.when(keep)
            def _():
                own[place] = value

            @pl.when(jnp.logical_not(keep))
            def _():
                part_out[place] = value.astype(BF16)
                copy().start()

        unit(bb, uu, j, take)
        waiting[place].append((keep, copy))
        return kb, uu, j, place

    def send_part(slot, place, uu):
        return pltpu.make_async_remote_copy(
            src_ref=part_out.at[place],
            dst_ref=part_in.at[slot, t],
            send_sem=ps_sem.at[place],
            recv_sem=pr_sem.at[slot, t],
            device_id=at(tensor=uu),
            device_id_type=pl.DeviceIdType.MESH,
        )

    def scatter(slot, kb, kc_, j):
        src = scat.at[slot, kc_]
        place = shift(b, (u - t + n_u), 2) * 2 + c
        index = (kb * 2 + kc_, j)
        return pltpu.make_async_remote_copy(
            src_ref=src,
            dst_ref=out.at[place, j],
            send_sem=ss_sem.at[index],
            recv_sem=sr_sem.at[index],
            device_id=at(b=shift(b, kb, 2), core=shift(c, kc_, 2)),
            device_id_type=pl.DeviceIdType.MESH,
        )

    def finish(kb, uu, j, place):
        slot = kb * N_CHUNK + j

        @pl.when(uu == t)
        def _():
            for k in range(1, n_u):
                frm = shift(t, k, n_u)
                pltpu.make_async_remote_copy(
                    src_ref=part_out.at[0],
                    dst_ref=part_in.at[slot, frm],
                    send_sem=ps_sem.at[0],
                    recv_sem=pr_sem.at[slot, frm],
                    device_id=t_to[k],
                    device_id_type=pl.DeviceIdType.MESH,
                ).wait_recv()
            for kc_ in range(2):
                at_c = pl.ds(pl.multiple_of(shift(c, kc_, 2) * rows, 16), rows)
                total = own[place, at_c, :]
                for k in range(1, n_u):
                    total = total + part_in[slot, shift(t, k, n_u), at_c, :].astype(F32)
                if kb == 0 and kc_ == 0:
                    out[shift(b, (u - t + n_u), 2) * 2 + c, j] = total.astype(BF16)
                else:
                    scat[slot, kc_] = total.astype(BF16)
                    scatter(slot, kb, kc_, j).start()

    pending = []

    def go(kb, ku, j):
        new = run_unit(kb, ku, j)
        if pending:
            finish(*pending.pop())
        pending.append(new)

    for load in loads:
        load.wait()
    h_core_in = hs.at[b, pl.ds(pl.multiple_of((1 - c) * rows, 16), rows), :]
    send(h, h_core_in, hc_sem, (0,), core_peer).wait_recv()
    relays = []

    def pass_h(i):
        got = h_rows(1 - b, c, i)
        send(got, got, hb_sem, (i,), b_peer).wait_recv()
        relay = send(got, got, hr_sem, (i,), core_peer)
        relay.start()
        relays.append(relay)

    passed = 0
    for j in range(N_CHUNK):
        while passed < H_CHUNK * (j + 1) // N_CHUNK:
            pass_h(passed)
            passed += 1
        for k in range(1, n_x):
            frm = shift(x, n_x - k, n_x)
            send(w_rows(u, frm, j), w_rows(u, frm, j), wx_sem, (k - 1, j), x_to[k]).wait_recv()
        go(0, 0, j)
    for i in range(H_CHUNK):
        got = h_rows(1 - b, 1 - c, i)
        send(got, got, hr_sem, (i,), core_peer).wait_recv()
    for j in range(N_CHUNK):
        go(1, 0, j)

    for k in range(1, n_u):
        frm_u = shift(u, n_u - k, n_u)

        def pass_w(j):
            got = w_rows(frm_u, x, j)
            send(got, got, wa_sem, (k - 1, j), u_to[k]).wait_recv()
            for m in range(1, n_x):
                relay = send(got, got, wr_sem, (k - 1, m - 1, j), x_to[m])
                relay.start()
                relays.append(relay)

        pass_w(0)
        for j in range(N_CHUNK):
            if j + 1 < N_CHUNK:
                pass_w(j + 1)
            for m in range(1, n_x):
                got = w_rows(frm_u, shift(x, n_x - m, n_x), j)
                send(got, got, wr_sem, (k - 1, m - 1, j), x_to[m]).wait_recv()
            for kb in range(2):
                go(kb, n_u - k, j)
    finish(*pending.pop())

    for place in range(2):
        for keep, copy in waiting[place]:

            @pl.when(jnp.logical_not(keep))
            def _():
                copy().wait_send()

    for copy in sent + relays + [h_core]:
        copy.wait_send()
    for kb in range(2):
        for kc_ in range(2):
            if kb or kc_:
                for j in range(N_CHUNK):
                    scatter(kb * N_CHUNK + j, kb, kc_, j).wait_send()
                    frm = shift(shift(b, kb, 2), (u - t + n_u), 2) * 2 + shift(c, kc_, 2)
                    index = (kb * 2 + kc_, j)
                    pltpu.make_async_remote_copy(
                        src_ref=out.at[frm, j],
                        dst_ref=out.at[frm, j],
                        send_sem=ss_sem.at[index],
                        recv_sem=sr_sem.at[index],
                        device_id=core_peer,
                        device_id_type=pl.DeviceIdType.MESH,
                    ).wait_recv()


def bulk(hidden, weight_t, n_u, n_x):
    rows, depth = hidden.shape
    cols = weight_t.shape[0]
    cw = cols // N_CHUNK
    wide = n_x * cw
    dma = pltpu.SemaphoreType.DMA
    few = max(n_x - 1, 1)
    return pl.pallas_call(
        functools.partial(bulk_kernel, n_u, n_x),
        out_shape=jax.ShapeDtypeStruct((4, N_CHUNK, rows, wide), BF16),
        in_specs=[pl.BlockSpec(memory_space=pltpu.HBM)] * 2,
        out_specs=pl.BlockSpec(memory_space=pltpu.VMEM),
        scratch_shapes=[
            pltpu.VMEM((2, 2 * rows, depth), BF16),
            pltpu.VMEM((n_u, n_x, cols, depth), BF16),
            pltpu.VMEM((2, 2 * rows, wide), F32),
            pltpu.VMEM((2, 2 * rows, wide), BF16),
            pltpu.VMEM((2 * N_CHUNK, n_u, 2 * rows, wide), BF16),
            pltpu.VMEM((2 * N_CHUNK, 2, rows, wide), BF16),
            dma((2,)),
            dma((2, 1)),
            dma((2, H_CHUNK)),
            dma((2, H_CHUNK)),
            dma((2, few, N_CHUNK)),
            dma((2, n_u - 1, N_CHUNK)),
            dma((2, n_u - 1, few, N_CHUNK)),
            dma((2,)),
            dma((2 * N_CHUNK, n_u)),
            dma((4, N_CHUNK)),
            dma((4, N_CHUNK)),
        ],
        compiler_params=pltpu.CompilerParams(
            collective_id=0, has_side_effects=True, vmem_limit_bytes=67043328
        ),
        name="bulk",
    )(hidden, weight_t)


def body(hidden, weight, factor_b, factor_a, magnitude, cotangent, *, n_u, n_x):
    rows, depth = hidden.shape
    cols = weight.shape[1]
    rank = factor_b.shape[1]
    out_cols = magnitude.shape[0]
    dp = ("u", "b", "x", "core")
    n_dp = n_u * 2 * n_x * 2
    own = lax.axis_index("tensor")

    low_part = jnp.dot(hidden, factor_b, preferred_element_type=F32)
    merged = weight.astype(F32) + jnp.dot(factor_b, factor_a, preferred_element_type=F32)
    local_sq = jnp.sum(merged * merged, axis=0)
    low, block_sq = lax.psum((low_part, local_sq), "tensor")
    col_sq = lax.all_gather(block_sq, dp, axis=0, tiled=True)
    full_a = lax.all_gather(factor_a, dp, axis=1, tiled=True)
    norms = jnp.sqrt(lax.dynamic_slice_in_dim(col_sq, own * out_cols, out_cols, 0) + 1e-06)
    scale = magnitude / norms
    low_b = low.astype(BF16)
    own_a = lax.dynamic_slice_in_dim(full_a, own * out_cols, out_cols, 1)
    adapter = jnp.dot(low_b, own_a, preferred_element_type=F32)

    cot = cotangent.astype(F32)
    dpre_b = (cot * scale).astype(BF16)
    back_b = lax.psum(jnp.dot(dpre_b, own_a.T, preferred_element_type=F32), "tensor").astype(BF16)
    b_part = jnp.dot(back_b.T, hidden, preferred_element_type=F32)
    a_part = jnp.dot(low_b.T, dpre_b, preferred_element_type=F32)
    parts = jnp.concatenate([v.reshape(rank, n_dp, -1) for v in (a_part, b_part)], axis=2)
    parts = lax.all_to_all(parts.transpose(1, 0, 2), dp, 0, 0, tiled=True)
    sums = jnp.sum(parts, axis=0)
    grad_a = sums[:, : out_cols // n_dp]
    grad_b = sums[:, out_cols // n_dp :].T

    got = bulk(hidden, weight.T, n_u, n_x)
    cw = cols // N_CHUNK
    got = got.reshape(2, 2, N_CHUNK, rows, n_x, cw).transpose(3, 0, 4, 1, 2, 5).reshape(rows, out_cols)
    pre = got.astype(F32) + adapter
    mixed = (pre * scale).astype(BF16)
    mag_part = jnp.sum(cot * pre, axis=0) / norms
    mag_part = lax.psum(mag_part, dp)
    me = lax.axis_index(dp)
    grad_scale = lax.dynamic_slice_in_dim(mag_part, me * (out_cols // n_dp), out_cols // n_dp, 0)
    return mixed, grad_scale, grad_a, grad_b


def solution(mesh):
    n_dp, n_u = mesh.shape["dp"], mesh.shape["tensor"]
    n_x = n_dp // (4 * n_u)
    fine = Mesh(mesh.devices.reshape(n_u, 2, n_x, 2, n_u), AXES)
    dp = ("u", "b", "x", "core")

    def step(*args):
        return body(*args, n_u=n_u, n_x=n_x)

    return jax.shard_map(
        step,
        mesh=fine,
        in_specs=(
            P(dp, "tensor"),
            P("tensor", dp),
            P("tensor", None),
            P(None, dp),
            P("tensor"),
            P(dp, "tensor"),
        ),
        out_specs=(
            P(dp, "tensor"),
            P(("tensor",) + dp),
            P(None, ("tensor",) + dp),
            P(("tensor",) + dp, None),
        ),
        check_vma=False,
    )
```

```python
import functools

import jax
import jax.numpy as jnp
from jax import lax
from jax.experimental import pallas as pl
from jax.experimental.pallas import tpu as pltpu
from jax.sharding import Mesh, PartitionSpec as P

F32, BF16 = jnp.float32, jnp.bfloat16
AXES = ("u", "b", "x", "core", "tensor")
MESH = pl.DeviceIdType.MESH
NT = (((1,), (1,)), ((), ()))
NN = (((1,), (0,)), ((), ()))
TN = (((0,), (0,)), ((), ()))
H_CHUNK = 4
PIECE = 64
LANES = 128


def split_of(size, most):
    best = LANES
    for step in range(LANES, most + 1, LANES):
        if size % step == 0:
            best = step
    return best


def cuts(size, step):
    return [(at, min(step, size - at)) for at in range(0, size, step)]


def granule(depth, n_dp):
    share = depth // n_dp
    size = share
    while size % LANES:
        size += share
    return size


def dot(left, right, dims):
    return lax.dot_general(left, right, dims, preferred_element_type=F32)


def kernel(
    n_u, n_x, h, w, bt, a, mag, cot, mixed, mag_out, ga_out, gb_out,
    hs, ws, own, part_out, part_in, scat, got_out, sq, sqx, low, lowx, back, backx, backs, pk, pks,
    ga, gax, gb, gbx, mg, mgx,
    loc_sem, hc_sem, hb_sem, hr_sem, wx_sem, wa_sem, wr_sem, ps_sem, pr_sem, sc_sem,
    sq_sem, low_sem, back_sem, tok_sem, pk_ssem, pk_rsem, ga_sem, gb_sem, mg_sem,
):
    u, b, x, c, t = (lax.axis_index(name) for name in AXES)
    rows, depth = h.shape
    cols = w.shape[0]
    rank = a.shape[0]
    n_blk = 4 * n_x
    n_dp = n_blk * n_u
    hr = rows // H_CHUNK
    kc = split_of(depth, 1152)
    chunks = cuts(cols, LANES)
    pieces = cuts(cols, PIECE)
    n_ch, n_pc = len(chunks), len(pieces)

    def at(**moved):
        here = dict(u=u, b=b, x=x, core=c, tensor=t)
        here.update(moved)
        return tuple(here[name] for name in AXES)

    def shift(value, by, n):
        return lax.rem(value + by, n)

    def remote(src, dst, send_sem, recv_sem, peer):
        return pltpu.make_async_remote_copy(
            src_ref=src, dst_ref=dst, send_sem=send_sem, recv_sem=recv_sem, device_id=peer, device_id_type=MESH
        )

    def send(src, dst, sems, index, peer):
        return remote(src, dst, sems.at[(0,) + index], sems.at[(1,) + index], peer)

    core_peer = at(core=1 - c)
    b_peer = at(b=1 - b)
    x_to = [at(x=shift(x, k, n_x)) for k in range(n_x)]
    u_to = [at(u=shift(u, k, n_u), b=shift(b, k % 2, 2)) for k in range(n_u)]
    t_to = [at(tensor=shift(t, k, n_u)) for k in range(n_u)]
    steps = [(i, j, k, l) for i in range(n_u) for j in range(2) for k in range(n_x) for l in range(2)]

    def moved(step):
        du, db, dx, dc = step
        return at(u=shift(u, du, n_u), b=shift(b, db, 2), x=shift(x, dx, n_x), core=shift(c, dc, 2))

    def place_of(device):
        return ((device[0] * 2 + device[1]) * n_x + device[2]) * 2 + device[3]

    def block_of(bb, xx, cc):
        return (bb * n_x + xx) * 2 + cc

    far = shift(b, u - t + n_u, 2)

    peers = [moved(step) for step in steps[1:]] + t_to[1:]
    barrier = pltpu.get_barrier_semaphore()
    for peer in peers:
        pl.semaphore_signal(barrier, inc=1, device_id=peer, device_id_type=MESH)
    pl.semaphore_wait(barrier, len(peers))

    def h_rows(bb, cc, i):
        return hs.at[bb, pl.ds(pl.multiple_of(cc * rows + i * hr, 16), hr), :]

    def w_rows(uu, xx, p):
        first, size = pieces[p]
        return ws.at[uu, xx, pl.ds(first, size), :]

    own_rows = hs.at[b, pl.ds(pl.multiple_of(c * rows, 16), rows), :]
    sent = []

    def start(copy):
        copy.start()
        sent.append(copy)

    def start_h(i):
        start(send(h.at[pl.ds(i * hr, hr), :], h_rows(b, c, i), hb_sem, (i,), b_peer))

    def start_wx(p):
        first, size = pieces[p]
        for k in range(1, n_x):
            start(send(w.at[pl.ds(first, size), :], w_rows(u, x, p), wx_sem, (k - 1, p), x_to[k]))

    def wa(k, p):
        first, size = pieces[p]
        return send(w.at[pl.ds(first, size), :], w_rows(u, x, p), wa_sem, (k - 1, p), u_to[k])

    def start_wa(p):
        for k in range(1, n_u):
            wa(k, p).start()

    early = u != b

    loads = [
        pltpu.make_async_copy(w, ws.at[u, x], loc_sem.at[1]),
        pltpu.make_async_copy(h, own_rows, loc_sem.at[0]),
    ]
    for load in loads:
        load.start()
    start(send(h, own_rows, hc_sem, (0,), core_peer))
    start_h(0)
    start_wx(0)

    @pl.when(early)
    def _():
        start_wa(0)

    loads[0].wait()
    a_t = jnp.transpose(a[...].astype(F32)).astype(BF16)

    def square_step(i, acc):
        at_k = pl.ds(pl.multiple_of(i * kc, LANES), kc)
        merged = ws[u, x, :, at_k].astype(F32) + dot(a_t, bt[:, at_k], NN)
        for g in range(kc // LANES):
            part = merged[:, g * LANES : (g + 1) * LANES]
            acc = acc + part * part
        return acc

    squares = lax.fori_loop(0, depth // kc, square_step, jnp.zeros((cols, LANES), F32))
    sq[...] = lax.dot_general(
        jnp.ones((8, LANES), F32), squares, NT, precision=lax.Precision.HIGHEST, preferred_element_type=F32
    )
    for k in range(1, n_u):
        start(send(sq, sqx.at[k - 1], sq_sem, (k - 1,), t_to[k]))

    loads[1].wait()

    def low_step(i, acc):
        at_k = pl.ds(pl.multiple_of(i * kc, LANES), kc)
        left = hs[b, pl.ds(pl.multiple_of(c * rows, 16), rows), at_k]
        return acc + dot(bt[:, at_k], left, NT)

    low[...] = lax.fori_loop(0, depth // kc, low_step, jnp.zeros((rank, rows), F32))
    for k in range(1, n_u):
        start(send(low, lowx.at[k - 1], low_sem, (k - 1,), t_to[k]))

    def from_t(ref, extra, sems):
        total = ref[...]
        for k in range(1, n_u):
            send(ref, extra.at[k - 1], sems, (k - 1,), t_to[k]).wait_recv()
            total = total + extra[k - 1]
        return total

    square_sum = from_t(sq, sqx, sq_sem)
    mine = block_of(b, x, c)

    def packet(n, step):
        return remote(
            pks, pk.at[mine], pk_ssem.at[n], pk_rsem.at[n % n_blk], moved(step)
        )

    @pl.when(u == t)
    def _():
        pks[0:rank, :] = a[...].astype(F32)
        pks[rank : rank + 8, :] = square_sum
        pk[mine, 0:rank, :] = a[...].astype(F32)
        pk[mine, rank : rank + 8, :] = square_sum
        for n, step in enumerate(steps):
            if n:
                packet(n, step).start()

    start_h(1)
    start_wx(1)

    @pl.when(early)
    def _():
        start_wa(1)

    low_t = from_t(low, lowx, low_sem)
    low_tb = low_t.astype(BF16)
    low_b = jnp.transpose(low_t).astype(BF16)

    count = [0]
    waiting = [[], []]

    def run_unit(kb, ku, j):
        first, size = chunks[j]
        wide = n_x * size
        place = count[0] % 2
        count[0] += 1
        bb, uu = shift(b, kb, 2), shift(u, ku, n_u)
        keep = uu == t
        slot = kb * n_ch + j

        def copy():
            lag = lax.rem(uu - t + n_u - 1 + n_u, n_u)
            return remote(
                part_out.at[place], part_in.at[slot, lag], ps_sem.at[place], pr_sem.at[slot, lag], at(tensor=uu)
            )

        if waiting[place]:
            old_keep, old_copy = waiting[place].pop()

            @pl.when(jnp.logical_not(old_keep))
            def _():
                old_copy().wait_send()

        own[place, :, 0:wide] = jnp.zeros((2 * rows, wide), F32)

        def unit_step(i, carry):
            at_k = pl.ds(pl.multiple_of(i * kc, LANES), kc)
            right = jnp.concatenate([ws[uu, xx, first : first + size, at_k] for xx in range(n_x)], axis=0)
            own[place, :, 0:wide] += dot(hs[bb, :, at_k], right, NT)
            return carry

        lax.fori_loop(0, depth // kc, unit_step, 0)

        @pl.when(jnp.logical_not(keep))
        def _():
            part_out[place, :, 0:wide] = own[place, :, 0:wide].astype(BF16)
            copy().start()

        waiting[place].append((keep, copy))
        return kb, uu, j, place

    def scatter(kb, kc_, j):
        index = (kb * 2 + kc_, j)
        return send(
            scat.at[kb * n_ch + j, kc_], got_out.at[far * 2 + c, j], sc_sem, index,
            at(b=shift(b, kb, 2), core=shift(c, kc_, 2)),
        )

    def finish(kb, uu, j, place):
        slot = kb * n_ch + j
        wide = n_x * chunks[j][1]

        @pl.when(uu == t)
        def _():
            for k in range(n_u - 1):
                remote(part_out.at[0], part_in.at[slot, k], ps_sem.at[0], pr_sem.at[slot, k], t_to[1]).wait_recv()
            for kc_ in range(2):
                at_c = pl.ds(pl.multiple_of(shift(c, kc_, 2) * rows, 16), rows)
                total = own[place, at_c, 0:wide]
                for k in range(n_u - 1):
                    total = total + part_in[slot, k, at_c, 0:wide].astype(F32)
                if kb == 0 and kc_ == 0:
                    got_out[far * 2 + c, j, :, 0:wide] = total.astype(BF16)
                else:
                    scat[slot, kc_, :, 0:wide] = total.astype(BF16)
                    scatter(kb, kc_, j).start()

    pending = []

    def go(kb, ku, j):
        new = run_unit(kb, ku, j)
        if pending:
            finish(*pending.pop())
        pending.append(new)

    passed = [0]

    def pass_h():
        i = passed[0]
        passed[0] += 1
        got = h_rows(1 - b, c, i)
        send(got, got, hb_sem, (i,), b_peer).wait_recv()
        start(send(got, got, hr_sem, (i,), core_peer))

    def near(p):
        for k in range(1, n_x):
            got = w_rows(u, shift(x, n_x - k, n_x), p)
            send(got, got, wx_sem, (k - 1, p), x_to[k]).wait_recv()

    def of_chunk(j):
        first, size = chunks[j]
        return [p for p in range(n_pc) if first <= pieces[p][0] < first + size]

    for q in range(n_blk):
        _, db, dx, dc = steps[q]
        src = block_of(shift(b, db, 2), shift(x, n_x - dx, n_x), shift(c, dc, 2))
        wait = remote(pks, pk.at[src], pk_ssem.at[0], pk_rsem.at[q], core_peer)
        if q:
            wait.wait_recv()
        else:
            pl.when(u != t)(wait.wait_recv)

    def scale_of(i, first, size):
        norm = jnp.sqrt(pk[i, rank : rank + 1, first : first + size] + 1e-06)
        return mag[:, i * cols + first : i * cols + first + size] / norm

    back_part = jnp.zeros((rank, rows), F32)
    for i in range(n_blk):
        piece = cot[:, i * cols : (i + 1) * cols].astype(F32)
        dpre = (piece * scale_of(i, 0, cols)).astype(BF16)
        back_part = back_part + dot(pk[i, 0:rank, :].astype(BF16), dpre, NT)
        ga[i] = dot(low_tb, dpre, NN).astype(BF16)
    back[...] = back_part
    for k in range(1, n_u):
        start(send(back, backx.at[k - 1], back_sem, (k - 1,), t_to[k]))
    for n, step in enumerate(steps):
        if n:
            peer = moved(step)
            start(send(ga.at[lax.div(place_of(peer), n_u)], gax.at[n], ga_sem, (n,), peer))
    back_b = from_t(back, backx, back_sem).astype(BF16)
    backs[b * 2 + c] = back_b
    for k in range(1, 4):
        peer = at(b=shift(b, k // 2, 2), core=shift(c, k % 2, 2))
        start(send(backs.at[b * 2 + c], backs.at[b * 2 + c], tok_sem, (k - 1,), peer))

    for i in range(2, H_CHUNK):
        start_h(i)
    for p in range(2, n_pc):
        start_wx(p)

    @pl.when(early)
    def _():
        for p in range(2, n_pc):
            start_wa(p)

    @pl.when(jnp.logical_not(early))
    def _():
        for p in range(2):
            start_wa(p)

    h_core_in = hs.at[b, pl.ds(pl.multiple_of((1 - c) * rows, 16), rows), :]
    send(h, h_core_in, hc_sem, (0,), core_peer).wait_recv()
    for j in range(n_ch):
        while passed[0] < H_CHUNK * (j + 1) // n_ch:
            pass_h()
        for p in of_chunk(j):
            near(p)
        go(0, 0, j)
    for i in range(H_CHUNK):
        got = h_rows(1 - b, 1 - c, i)
        send(got, got, hr_sem, (i,), core_peer).wait_recv()

    for k in range(1, 4):
        src = shift(b, k // 2, 2) * 2 + shift(c, k % 2, 2)
        send(backs.at[src], backs.at[src], tok_sem, (k - 1,), core_peer).wait_recv()

    def grad_step(i, carry):
        at_k = pl.ds(pl.multiple_of(i * kc, LANES), kc)
        total = jnp.zeros((rank, kc), F32)
        for bb in range(2):
            for cc in range(2):
                total = total + dot(backs[bb * 2 + cc], hs[bb, cc * rows : (cc + 1) * rows, at_k], NN)
        gb[:, at_k] = total
        return carry

    lax.fori_loop(0, depth // kc, grad_step, 0)
    size_b = granule(depth, n_dp)
    share_b = depth // n_dp

    def lanes_of(device):
        return pl.ds(pl.multiple_of(lax.div(place_of(device) * share_b, size_b) * size_b, LANES), size_b)

    groups = [step for step in steps if step[1] == 0 and step[3] == 0]
    for n, step in enumerate(groups):
        if n:
            peer = moved(step)
            start(send(gb.at[:, lanes_of(peer)], gbx.at[n], gb_sem, (n,), peer))

    @pl.when(jnp.logical_not(early))
    def _():
        for p in range(2, n_pc):
            start_wa(p)

    for j in range(n_ch):
        go(1, 0, j)

    for k in range(1, n_u):
        frm_u = shift(u, n_u - k, n_u)

        def pass_w(j):
            for p in of_chunk(j):
                got = w_rows(frm_u, x, p)
                send(got, got, wa_sem, (k - 1, p), u_to[k]).wait_recv()
                for m in range(1, n_x):
                    start(send(got, got, wr_sem, (k - 1, m - 1, p), x_to[m]))

        pass_w(0)
        for j in range(n_ch):
            if j + 1 < n_ch:
                pass_w(j + 1)
            for p in of_chunk(j):
                for m in range(1, n_x):
                    got = w_rows(frm_u, shift(x, n_x - m, n_x), p)
                    send(got, got, wr_sem, (k - 1, m - 1, p), x_to[m]).wait_recv()
            for kb in range(2):
                go(kb, n_u - k, j)
    finish(*pending.pop())

    for bb in range(2):
        for cc in range(2):
            for j, (first, size) in enumerate(chunks):
                slot = bb * 2 + cc

                @pl.when(jnp.logical_or(bb != far, cc != c))
                def _():
                    kind = lax.rem(bb + far, 2) * 2 + lax.rem(cc + c, 2)
                    got = got_out.at[slot, j]
                    send(got, got, sc_sem, (kind, j), core_peer).wait_recv()

                for xx in range(n_x):
                    i = block_of(bb, xx, cc)
                    left = i * cols + first
                    pre = got_out[slot, j, :, xx * size : (xx + 1) * size].astype(F32)
                    pre = pre + dot(low_b, pk[i, 0:rank, first : first + size].astype(BF16), NN)
                    mixed[:, left : left + size] = (pre * scale_of(i, first, size)).astype(BF16)
                    part = jnp.sum(cot[:, left : left + size].astype(F32) * pre, axis=0, keepdims=True)
                    mg[i, 0:1, first : first + size] = part
    for n, step in enumerate(steps):
        if n:
            peer = moved(step)
            start(send(mg.at[lax.div(place_of(peer), n_u)], mgx.at[n], mg_sem, (n,), peer))

    block = lax.div(place_of(at()), n_u)
    total = ga[block].astype(F32)
    for n in range(1, n_dp):
        send(ga.at[0], gax.at[n], ga_sem, (n,), core_peer).wait_recv()
        total = total + gax[n].astype(F32)
    ga_out[...] = total
    total = gb[:, lanes_of(at())]
    for n in range(1, len(groups)):
        send(gbx.at[0], gbx.at[n], gb_sem, (n,), core_peer).wait_recv()
        total = total + gbx[n]
    gb_out[...] = total

    for place in range(2):
        for keep, copy in waiting[place]:

            @pl.when(jnp.logical_not(keep))
            def _():
                copy().wait_send()

    @pl.when(u == t)
    def _():
        for n, step in enumerate(steps):
            if n:
                packet(n, step).wait_send()

    for k in range(1, n_u):
        for p in range(n_pc):
            wa(k, p).wait_send()
    for kb in range(2):
        for kc_ in range(2):
            if kb or kc_:
                for j in range(n_ch):
                    scatter(kb, kc_, j).wait_send()
    for copy in sent:
        copy.wait_send()

    total = mg[block]
    for n in range(1, n_dp):
        send(mg.at[0], mgx.at[n], mg_sem, (n,), core_peer).wait_recv()
        total = total + mgx[n]
    mag_out[...] = total[0:1] / jnp.sqrt(pk[block, rank : rank + 1, :] + 1e-06)


def fused(hidden, weight_t, factor_bt, factor_a, magnitude, cotangent, n_u, n_x):
    rows, depth = hidden.shape
    cols = weight_t.shape[0]
    rank = factor_a.shape[0]
    n_blk = 4 * n_x
    n_dp = n_blk * n_u
    n_ch, n_pc = len(cuts(cols, LANES)), len(cuts(cols, PIECE))
    wide = n_x * LANES
    size_b = granule(depth, n_dp)
    groups = n_u * n_x
    few = max(n_x - 1, 1)
    sem = pltpu.SemaphoreType.DMA
    vmem = pltpu.VMEM
    whole = pl.BlockSpec(memory_space=pltpu.VMEM)
    return pl.pallas_call(
        functools.partial(kernel, n_u, n_x),
        out_shape=(
            jax.ShapeDtypeStruct(cotangent.shape, BF16),
            jax.ShapeDtypeStruct((1, cols), F32),
            jax.ShapeDtypeStruct((rank, cols), F32),
            jax.ShapeDtypeStruct((rank, size_b), F32),
        ),
        in_specs=[pl.BlockSpec(memory_space=pltpu.HBM)] * 2 + [whole] * 4,
        out_specs=(whole,) * 4,
        scratch_shapes=[
            vmem((2, 2 * rows, depth), BF16),
            vmem((n_u, n_x, cols, depth), BF16),
            vmem((2, 2 * rows, wide), F32),
            vmem((2, 2 * rows, wide), BF16),
            vmem((2 * n_ch, n_u - 1, 2 * rows, wide), BF16),
            vmem((2 * n_ch, 2, rows, wide), BF16),
            vmem((4, n_ch, rows, wide), BF16),
            vmem((8, cols), F32),
            vmem((n_u - 1, 8, cols), F32),
            vmem((rank, rows), F32),
            vmem((n_u - 1, rank, rows), F32),
            vmem((rank, rows), F32),
            vmem((n_u - 1, rank, rows), F32),
            vmem((4, rank, rows), BF16),
            vmem((n_blk, rank + 8, cols), F32),
            vmem((rank + 8, cols), F32),
            vmem((n_blk, rank, cols), BF16),
            vmem((n_dp, rank, cols), BF16),
            vmem((rank, depth), F32),
            vmem((groups, rank, size_b), F32),
            vmem((n_blk, 8, cols), F32),
            vmem((n_dp, 8, cols), F32),
            sem((2,)),
            sem((2, 1)),
            sem((2, H_CHUNK)),
            sem((2, H_CHUNK)),
            sem((2, few, n_pc)),
            sem((2, n_u - 1, n_pc)),
            sem((2, n_u - 1, few, n_pc)),
            sem((2,)),
            sem((2 * n_ch, n_u - 1)),
            sem((2, 4, n_ch)),
            sem((2, n_u - 1)),
            sem((2, n_u - 1)),
            sem((2, n_u - 1)),
            sem((2, 3)),
            sem((n_dp,)),
            sem((n_blk,)),
            sem((2, n_dp)),
            sem((2, groups)),
            sem((2, n_dp)),
        ],
        compiler_params=pltpu.CompilerParams(
            collective_id=0, has_side_effects=True, vmem_limit_bytes=67043328
        ),
        name="fused",
    )(hidden, weight_t, factor_bt, factor_a, magnitude, cotangent)


def body(hidden, weight, factor_b, factor_a, magnitude, cotangent, *, n_u, n_x):
    depth = hidden.shape[1]
    cols = weight.shape[1]
    n_dp = n_u * 4 * n_x
    mixed, mag, ga, gb = fused(
        hidden, weight.T, factor_b.T, factor_a, magnitude[None], cotangent, n_u, n_x
    )
    me = lax.axis_index(("u", "b", "x", "core"))
    share = cols // n_u
    first = lax.rem(me, n_u) * share
    share_b = depth // n_dp
    first_b = lax.rem(me * share_b, gb.shape[1])
    return (
        mixed,
        lax.dynamic_slice_in_dim(mag[0], first, share, 0),
        lax.dynamic_slice_in_dim(ga, first, share, 1),
        lax.dynamic_slice_in_dim(gb, first_b, share_b, 1).T,
    )


def solution(mesh):
    n_dp, n_u = mesh.shape["dp"], mesh.shape["tensor"]
    n_x = n_dp // (4 * n_u)
    fine = Mesh(mesh.devices.reshape(n_u, 2, n_x, 2, n_u), AXES)
    dp = ("u", "b", "x", "core")

    def step(*args):
        return body(*args, n_u=n_u, n_x=n_x)

    return jax.shard_map(
        step,
        mesh=fine,
        in_specs=(
            P(dp, "tensor"),
            P("tensor", dp),
            P("tensor", None),
            P(None, dp),
            P("tensor"),
            P(dp, "tensor"),
        ),
        out_specs=(
            P(dp, "tensor"),
            P(("tensor",) + dp),
            P(None, ("tensor",) + dp),
            P(("tensor",) + dp, None),
        ),
        check_vma=False,
    )
```

```python
import functools

import jax
import jax.numpy as jnp
from jax import lax
from jax.experimental import pallas as pl
from jax.experimental.pallas import tpu as pltpu
from jax.sharding import Mesh, PartitionSpec as P

F32, BF16 = jnp.float32, jnp.bfloat16
AXES = ("u", "b", "x", "core", "tensor")
MESH = pl.DeviceIdType.MESH
NT = (((1,), (1,)), ((), ()))
NN = (((1,), (0,)), ((), ()))
TN = (((0,), (0,)), ((), ()))
H_CHUNK = 6
LATE_CHUNK = 2
LATE_SHARE = 10
PIECE = 32
LANES = 128


def split_of(size, most):
    best = LANES
    for step in range(LANES, most + 1, LANES):
        if size % step == 0:
            best = step
    return best


def cuts(size, step):
    return [(at, min(step, size - at)) for at in range(0, size, step)]


def chunks_of(cols, n_x):
    rest = cuts(cols - LANES, LANES // n_x)
    return [(0, LANES)] + [(LANES + at, size) for at, size in rest]


def pieces_of(cols, n_x):
    last = chunks_of(cols, n_x)[-1][0]
    return cuts(last, PIECE) + [(last + at, size) for at, size in cuts(cols - last, PIECE // 2)]


def granule(depth, n_dp):
    share = depth // n_dp
    size = share
    while size % LANES:
        size += share
    return size


def padded(lanes):
    return -(-lanes // LANES) * LANES


def dot(left, right, dims):
    return lax.dot_general(left, right, dims, preferred_element_type=F32)


def kernel(
    n_u, n_x, h, w, bt, a, mag, cot, mixed, mag_out, ga_out, gb_out,
    hs, ws, own, part_out, part_in, scat, late_sum, late_own, late_out, late_in, got_out, sq, sqx, low, lowx, back, backx, backs, pk_a, pk_s, pks,
    ga, gax, gb, gbx, mg, mgx,
    loc_sem, hc_sem, hb_sem, hr_sem, wx_sem, wa_sem, wr_sem, ps_sem, pr_sem, sc_sem, ls_sem, lr_sem, lsc_sem, turn_sem,
    sq_sem, low_sem, back_sem, tok_sem, pk_ssem, pk_rsem, ga_sem, gb_sem, mg_sem,
):
    u, b, x, c, t = (lax.axis_index(name) for name in AXES)
    rows, depth = h.shape
    cols = w.shape[0]
    rank = a.shape[0]
    n_blk = 4 * n_x
    n_dp = n_blk * n_u
    late = rows // LATE_SHARE
    soon = rows - late
    kc = split_of(depth, 1152)
    n_h = H_CHUNK + LATE_CHUNK
    h_cuts = [(i * (soon // H_CHUNK), soon // H_CHUNK) for i in range(H_CHUNK)]
    h_cuts += [(soon + i * (late // LATE_CHUNK), late // LATE_CHUNK) for i in range(LATE_CHUNK)]
    chunks = chunks_of(cols, n_x)
    pieces = pieces_of(cols, n_x)
    n_ch, n_pc = len(chunks), len(pieces)

    def at(**moved):
        here = dict(u=u, b=b, x=x, core=c, tensor=t)
        here.update(moved)
        return tuple(here[name] for name in AXES)

    def shift(value, by, n):
        return lax.rem(value + by, n)

    def remote(src, dst, send_sem, recv_sem, peer):
        return pltpu.make_async_remote_copy(
            src_ref=src, dst_ref=dst, send_sem=send_sem, recv_sem=recv_sem, device_id=peer, device_id_type=MESH
        )

    def send(src, dst, sems, index, peer):
        return remote(src, dst, sems.at[(0,) + index], sems.at[(1,) + index], peer)

    core_peer = at(core=1 - c)
    b_peer = at(b=1 - b)
    x_to = [at(x=shift(x, k, n_x)) for k in range(n_x)]
    u_to = [at(u=shift(u, k, n_u), b=shift(b, k % 2, 2)) for k in range(n_u)]
    t_to = [at(tensor=shift(t, k, n_u)) for k in range(n_u)]
    steps = [(i, j, k, l) for i in range(n_u) for j in range(2) for k in range(n_x) for l in range(2)]

    def moved(step):
        du, db, dx, dc = step
        return at(u=shift(u, du, n_u), b=shift(b, db, 2), x=shift(x, dx, n_x), core=shift(c, dc, 2))

    def place_of(device):
        return ((device[0] * 2 + device[1]) * n_x + device[2]) * 2 + device[3]

    def block_of(bb, xx, cc):
        return (bb * n_x + xx) * 2 + cc

    far = shift(b, u - t + n_u, 2)

    peers = [moved(step) for step in steps[1:]] + t_to[1:]
    barrier = pltpu.get_barrier_semaphore()
    for peer in peers:
        pl.semaphore_signal(barrier, inc=1, device_id=peer, device_id_type=MESH)
    pl.semaphore_wait(barrier, len(peers))

    def row_of(kb, cc, first):
        return kb * 2 * rows + (cc * soon + first if first < soon else 2 * soon + cc * late + first - soon)

    def rows_at(kb, cc, first, size):
        return pl.ds(pl.multiple_of(row_of(kb, cc, first), 16), size)

    halves = [(0, soon), (soon, late)]

    def h_rows(kb, cc, i):
        return hs.at[rows_at(kb, cc, *h_cuts[i]), :]

    def w_rows(uu, xx, p):
        first, size = pieces[p]
        return ws.at[uu, xx, pl.ds(first, size), :]

    def half_rows(cc, half):
        return hs.at[rows_at(0, cc, *halves[half]), :]

    sent = []

    def start(copy):
        copy.start()
        sent.append(copy)

    def late_h(i):
        return send(h.at[pl.ds(*h_cuts[i]), :], h_rows(1, c, i), hb_sem, (i,), b_peer)

    def start_h(i):
        start(late_h(i))

    def start_wx(p):
        first, size = pieces[p]
        for k in range(1, n_x):
            start(send(w.at[pl.ds(first, size), :], w_rows(u, x, p), wx_sem, (k - 1, p), x_to[k]))

    def wa(k, p):
        first, size = pieces[p]
        return send(w.at[pl.ds(first, size), :], w_rows(u, x, p), wa_sem, (k - 1, p), u_to[k])

    def start_wa(p):
        for k in range(1, n_u):
            wa(k, p).start()

    early = lax.rem(u, 2) != b

    loads = [
        pltpu.make_async_copy(w, ws.at[u, x], loc_sem.at[1]),
    ] + [
        pltpu.make_async_copy(h.at[pl.ds(*halves[i]), :], half_rows(c, i), loc_sem.at[2 * i]) for i in range(2)
    ]
    for load in loads:
        load.start()
    for i in range(2):
        start(send(h.at[pl.ds(*halves[i]), :], half_rows(c, i), hc_sem, (i,), core_peer))
    start_h(0)
    for p in range(2):
        start_wx(p)

    @pl.when(early)
    def _():
        for p in range(2):
            start_wa(p)

    loads[0].wait()
    a_t = jnp.transpose(a[...].astype(F32)).astype(BF16)

    def square_step(i, acc):
        at_k = pl.ds(pl.multiple_of(i * kc, LANES), kc)
        merged = ws[u, x, :, at_k].astype(F32) + dot(a_t, bt[:, at_k], NN)
        for g in range(kc // LANES):
            part = merged[:, g * LANES : (g + 1) * LANES]
            acc = acc + part * part
        return acc

    squares = lax.fori_loop(0, depth // kc, square_step, jnp.zeros((cols, LANES), F32))
    sq[...] = lax.dot_general(
        jnp.ones((8, LANES), F32), squares, NT, precision=lax.Precision.HIGHEST, preferred_element_type=F32
    )
    for k in range(1, n_u):
        start(send(sq, sqx.at[k - 1], sq_sem, (k - 1,), t_to[k]))

    loads[1].wait()
    loads[2].wait()

    def low_step(i, acc):
        at_k = pl.ds(pl.multiple_of(i * kc, LANES), kc)
        left = jnp.concatenate([hs[rows_at(0, c, *half), at_k] for half in halves], axis=0)
        return acc + dot(bt[:, at_k], left, NT)

    low[...] = lax.fori_loop(0, depth // kc, low_step, jnp.zeros((rank, rows), F32))
    for k in range(1, n_u):
        start(send(low, lowx.at[k - 1], low_sem, (k - 1,), t_to[k]))

    def from_t(ref, extra, sems):
        total = ref[...]
        for k in range(1, n_u):
            send(ref, extra.at[k - 1], sems, (k - 1,), t_to[k]).wait_recv()
            total = total + extra[k - 1]
        return total

    square_sum = from_t(sq, sqx, sq_sem)
    mine = block_of(b, x, c)

    def packet(n, step):
        return [
            remote(a, pk_a.at[mine], pk_ssem.at[0, n], pk_rsem.at[0, n % n_blk], moved(step)),
            remote(pks, pk_s.at[mine], pk_ssem.at[1, n], pk_rsem.at[1, n % n_blk], moved(step)),
        ]

    @pl.when(u == t)
    def _():
        pks[...] = square_sum[0:1, :]
        pk_a[mine] = a[...]
        pk_s[mine] = square_sum[0:1, :]
        for n, step in enumerate(steps):
            if n:
                for copy in packet(n, step):
                    copy.start()

    for i in range(1, 3):
        start_h(i)
    for p in range(2, 4):
        start_wx(p)

    @pl.when(early)
    def _():
        for p in range(2, 4):
            start_wa(p)

    low_t = from_t(low, lowx, low_sem)
    low_tb = low_t.astype(BF16)
    low_b = jnp.transpose(low_t).astype(BF16)

    count = [0]
    waiting = [[], []]

    def lag_of(uu):
        return lax.rem(uu - t + 2 * n_u - 1, n_u)

    def lanes_in(j):
        first, size = chunks[j]
        return pl.ds(n_x * first, padded(n_x * size))

    spans = {0: (0, 2 * rows), 1: (2 * rows, 2 * soon), 2: (0, 2 * (rows + soon))}

    def run_unit(kb, ku, j):
        first, size = chunks[j]
        wide = n_x * size
        top, tall = spans[kb]
        place = count[0] % 2
        count[0] += 1
        uu = shift(u, ku, n_u)
        keep = uu == t

        def copy():
            return remote(
                part_out.at[place, 0:tall, 0 : padded(wide)], part_in.at[lag_of(uu), top : top + tall, lanes_in(j)],
                ps_sem.at[place], pr_sem.at[min(kb, 1), j, lag_of(uu)], at(tensor=uu),
            )

        if waiting[place]:
            old_keep, old_copy = waiting[place].pop()

            @pl.when(jnp.logical_not(old_keep))
            def _():
                old_copy().wait_send()

        own[place, 0:tall, 0:wide] = jnp.zeros((tall, wide), F32)

        def unit_step(i, carry):
            at_k = pl.ds(pl.multiple_of(i * kc, LANES), kc)
            right = jnp.concatenate([ws[uu, xx, first : first + size, at_k] for xx in range(n_x)], axis=0)
            own[place, 0:tall, 0:wide] += dot(hs[top : top + tall, at_k], right, NT)
            return carry

        lax.fori_loop(0, depth // kc, unit_step, 0)

        @pl.when(jnp.logical_not(keep))
        def _():
            part_out[place, 0:tall, 0:wide] = own[place, 0:tall, 0:wide].astype(BF16)
            copy().start()

        waiting[place].append((keep, copy))
        return kb, uu, j, place

    def scatter(kb, kc_, j):
        index = (kb * 2 + kc_, j)
        span = pl.ds(0, soon if kb else rows)
        return send(
            scat.at[kb * 2 + kc_, span, lanes_in(j)], got_out.at[far * 2 + c, span, lanes_in(j)], sc_sem, index,
            at(b=shift(b, kb, 2), core=shift(c, kc_, 2)),
        )

    def finish(kb, uu, j, place):
        first, size = chunks[j]
        wide = n_x * size
        top, tall = spans[kb]
        lanes = pl.ds(n_x * first, wide)

        @pl.when(uu == t)
        def _():
            for k in range(n_u - 1):
                remote(
                    part_out.at[0, 0:tall, 0 : padded(wide)], part_in.at[k, top : top + tall, lanes_in(j)],
                    ps_sem.at[0], pr_sem.at[min(kb, 1), j, k], t_to[1],
                ).wait_recv()
            for side in (0, 1) if kb == 2 else (kb,):
                for kc_ in range(2):
                    for half in halves[: 1 if side else 2]:
                        at_c = row_of(side, shift(c, kc_, 2), half[0])
                        total = own[place, pl.ds(pl.multiple_of(at_c - top, 16), half[1]), 0:wide]
                        for k in range(n_u - 1):
                            more = part_in[k, pl.ds(pl.multiple_of(at_c, 16), half[1]), lanes]
                            total = total + more.astype(F32)
                        if side == 0 and kc_ == 0:
                            got_out[far * 2 + c, pl.ds(*half), lanes] = total.astype(BF16)
                        else:
                            scat[side * 2 + kc_, pl.ds(*half), lanes] = total.astype(BF16)
                    if side or kc_:
                        scatter(side, kc_, j).start()

    pending = []

    def go(kb, ku, j):
        new = run_unit(kb, ku, j)
        if pending:
            finish(*pending.pop())
        pending.append(new)

    def late_part(uu):
        return remote(late_out, late_in.at[lag_of(uu)], ls_sem.at[0], lr_sem.at[lag_of(uu)], at(tensor=uu))

    def late_unit(uu):
        late_sum[...] = jnp.zeros(late_sum.shape, F32)

        def late_step(i, carry):
            at_k = pl.ds(pl.multiple_of(i * kc, LANES), kc)
            right = jnp.concatenate(
                [ws[uu, xx, first : first + size, at_k] for first, size in chunks for xx in range(n_x)], axis=0
            )
            late_sum[...] += dot(right, hs[2 * (rows + soon) : 4 * rows, at_k], NT)
            return carry

        lax.fori_loop(0, depth // kc, late_step, 0)
        return jnp.transpose(late_sum[...])

    def late_scatter(kc_):
        return send(
            scat.at[2 + kc_, pl.ds(soon, late), :], got_out.at[far * 2 + c, pl.ds(soon, late), :], lsc_sem, (kc_,),
            at(b=1 - b, core=shift(c, kc_, 2)),
        )

    passed = [0]

    def pass_h():
        i = passed[0]
        passed[0] += 1
        got = h_rows(1, c, i)
        send(got, got, hb_sem, (i,), b_peer).wait_recv()
        start(send(got, got, hr_sem, (i,), core_peer))

    def near(p):
        for k in range(1, n_x):
            got = w_rows(u, shift(x, n_x - k, n_x), p)
            send(got, got, wx_sem, (k - 1, p), x_to[k]).wait_recv()

    def of_chunk(j):
        first, size = chunks[j]
        return [p for p in range(n_pc) if first <= pieces[p][0] < first + size]

    for q in range(n_blk):
        _, db, dx, dc = steps[q]
        src = block_of(shift(b, db, 2), shift(x, n_x - dx, n_x), shift(c, dc, 2))
        for wait in (
            remote(a, pk_a.at[src], pk_ssem.at[0, 0], pk_rsem.at[0, q], core_peer),
            remote(pks, pk_s.at[src], pk_ssem.at[1, 0], pk_rsem.at[1, q], core_peer),
        ):
            if q:
                wait.wait_recv()
            else:
                pl.when(u != t)(wait.wait_recv)

    def scale_of(i, first, size):
        norm = jnp.sqrt(pk_s[i, 0:1, first : first + size] + 1e-06)
        return mag[:, i * cols + first : i * cols + first + size] / norm

    back_part = jnp.zeros((rank, rows), F32)
    for i in range(n_blk):
        piece = cot[:, i * cols : (i + 1) * cols].astype(F32)
        dpre = (piece * scale_of(i, 0, cols)).astype(BF16)
        back_part = back_part + dot(pk_a[i], dpre, NT)
        ga[i] = dot(low_tb, dpre, NN).astype(BF16)
    back[...] = back_part
    for k in range(1, n_u):
        start(send(back, backx.at[k - 1], back_sem, (k - 1,), t_to[k]))
    for n, step in enumerate(steps):
        if n:
            peer = moved(step)
            start(send(ga.at[lax.div(place_of(peer), n_u)], gax.at[n], ga_sem, (n,), peer))
    back_b = from_t(back, backx, back_sem).astype(BF16)
    backs[c] = back_b
    for k in range(1, 4):
        peer = at(b=shift(b, k // 2, 2), core=shift(c, k % 2, 2))
        start(send(backs.at[c], backs.at[k // 2 * 2 + c], tok_sem, (k - 1,), peer))

    for i in range(3, H_CHUNK):
        start_h(i)
    for p in range(4, n_pc):
        start_wx(p)

    @pl.when(early)
    def _():
        for p in range(4, n_pc):
            start_wa(p)

    for i in range(2):
        send(half_rows(1 - c, i), half_rows(1 - c, i), hc_sem, (i,), core_peer).wait_recv()

    def turn(peer):
        pl.semaphore_signal(turn_sem, inc=1, device_id=peer, device_id_type=MESH)

    def w_arrived(k, p):
        got = w_rows(shift(u, n_u - k, n_u), x, p)
        send(got, got, wa_sem, (k - 1, p), u_to[k]).wait_recv()
        for m in range(1, n_x):
            send(got, got, wr_sem, (k - 1, m - 1, p), x_to[m]).start()

    for j in range(n_ch):
        while passed[0] < H_CHUNK * (j + 1) // n_ch:
            pass_h()
        for p in of_chunk(j):
            near(p)
        if j >= n_ch - 2:

            @pl.when(early)
            def _():
                for k in range(1, n_u):
                    for p in range(n_pc):
                        if (p in of_chunk(n_ch - 1)) == (j == n_ch - 1):
                            w_arrived(k, p)
                if j == n_ch - 1:
                    turn(at(u=shift(u, 1, n_u)))

        if j == n_ch - 1:

            @pl.when(jnp.logical_not(early))
            def _():
                pl.semaphore_wait(turn_sem, 1)
                for p in range(n_pc):
                    start_wa(p)
                for i in range(H_CHUNK, n_h):
                    late_h(i).start()

        go(0, 0, j)
    for i in range(H_CHUNK):
        got = h_rows(1, 1 - c, i)
        send(got, got, hr_sem, (i,), core_peer).wait_recv()

    for k in range(1, 4):
        src = k // 2 * 2 + shift(c, k % 2, 2)
        send(backs.at[src], backs.at[src], tok_sem, (k - 1,), core_peer).wait_recv()

    def grad_of(kb, half, at_k):
        first, size = halves[half]
        total = jnp.zeros((rank, kc), F32)
        for cc in range(2):
            held = hs[row_of(kb, cc, first) : row_of(kb, cc, first) + size, at_k]
            total = total + dot(backs[kb * 2 + cc, :, first : first + size], held, NN)
        return total

    def grad_step(i, carry):
        at_k = pl.ds(pl.multiple_of(i * kc, LANES), kc)
        total = jnp.zeros((rank, kc), F32)
        for kb, half in ((0, 0), (0, 1), (1, 0)):
            total = total + grad_of(kb, half, at_k)
        gb[:, at_k] = total
        return carry

    lax.fori_loop(0, depth // kc, grad_step, 0)
    size_b = granule(depth, n_dp)
    share_b = depth // n_dp

    def lanes_of(device):
        return pl.ds(pl.multiple_of(lax.div(place_of(device) * share_b, size_b) * size_b, LANES), size_b)

    groups = [step for step in steps if step[1] == 0 and step[3] == 0]
    def far_piece(k, p):
        @pl.when(jnp.logical_not(early))
        def _():
            w_arrived(k, p)
            if k == n_u - 1 and p == n_pc - 1:
                turn(b_peer)

    def far_ready(k, j):
        for p in of_chunk(j):
            for m in range(1, n_x):
                got = w_rows(shift(u, n_u - k, n_u), shift(x, n_x - m, n_x), p)
                send(got, got, wr_sem, (k - 1, m - 1, p), x_to[m]).wait_recv()

    units = [(1, 0, j) for j in range(n_ch)]
    for k in range(1, n_u):
        for p in range(n_pc):
            done = [j for j in range(n_ch) if max(of_chunk(j)) == p - 1]
            if units and not (k == n_u - 1 and p == n_pc - 1):
                go(*units.pop(0))
            far_piece(k, p)
            for j in done:
                far_ready(k, j)
                units.append((2, n_u - k, j))
        if k == n_u - 1:
            while units:
                go(*units.pop(0))

            @pl.when(early)
            def _():
                pl.semaphore_wait(turn_sem, 1)
                for i in range(H_CHUNK, n_h):
                    late_h(i).start()

        far_ready(k, n_ch - 1)
        units.append((2, n_u - k, n_ch - 1))
    for unit in units:
        go(*unit)
    finish(*pending.pop())

    for i in range(H_CHUNK, n_h):
        pass_h()
    for i in range(H_CHUNK, n_h):
        got = h_rows(1, 1 - c, i)
        send(got, got, hr_sem, (i,), core_peer).wait_recv()
    for k in range(1, n_u):
        if k > 1:
            late_part(shift(t, k - 1, n_u)).wait_send()
        late_out[:, 0 : n_x * cols] = late_unit(shift(t, k, n_u)).astype(BF16)
        late_part(shift(t, k, n_u)).start()

    def grad_late(i, carry):
        at_k = pl.ds(pl.multiple_of(i * kc, LANES), kc)
        gb[:, at_k] += grad_of(1, 1, at_k)
        return carry

    lax.fori_loop(0, depth // kc, grad_late, 0)
    for n, step in enumerate(groups):
        if n:
            peer = moved(step)
            start(send(gb.at[:, lanes_of(peer)], gbx.at[n], gb_sem, (n,), peer))
    late_own[:, 0 : n_x * cols] = late_unit(t)

    def emit(bb, cc, j, half):
        first, size = chunks[j]
        span = pl.ds(*halves[half])
        for xx in range(n_x):
            i = block_of(bb, xx, cc)
            left = i * cols + first
            lane = n_x * first + xx * size
            pre = got_out[bb * 2 + cc, span, lane : lane + size].astype(F32)
            low_half = low_b[halves[half][0] : sum(halves[half]), :]
            pre = pre + dot(low_half, pk_a[i, :, first : first + size], NN)
            mixed[span, left : left + size] = (pre * scale_of(i, first, size)).astype(BF16)
            part = jnp.sum(cot[span, left : left + size].astype(F32) * pre, axis=0, keepdims=True)
            if half:
                mg[i, 0:1, first : first + size] += part
            else:
                mg[i, 0:1, first : first + size] = part

    def soon_outputs(bb):
        for cc in range(2):
            for j in range(n_ch):
                kind = lax.rem(bb + far, 2) * 2 + lax.rem(cc + c, 2)

                def scattered(span):
                    got = got_out.at[bb * 2 + cc, span, lanes_in(j)]
                    return send(got, got, sc_sem, (kind, j), core_peer)

                @pl.when(jnp.logical_and(bb == far, cc != c))
                def _():
                    scattered(pl.ds(0, rows)).wait_recv()

                @pl.when(bb != far)
                def _():
                    scattered(pl.ds(0, soon)).wait_recv()

                emit(bb, cc, j, 0)

                @pl.when(bb == far)
                def _():
                    emit(bb, cc, j, 1)

    soon_outputs(0)
    for k in range(n_u - 1):
        remote(late_out, late_in.at[k], ls_sem.at[0], lr_sem.at[k], t_to[1]).wait_recv()
    for kc_ in range(2):
        at_c = pl.ds(pl.multiple_of(shift(c, kc_, 2) * late, 16), late)
        total = late_own[at_c, 0 : n_x * cols]
        for k in range(n_u - 1):
            total = total + late_in[k, at_c, 0 : n_x * cols].astype(F32)
        scat[2 + kc_, pl.ds(soon, late), 0 : n_x * cols] = total.astype(BF16)
        late_scatter(kc_).start()
    soon_outputs(1)
    for kc_ in range(2):
        got = got_out.at[(1 - far) * 2 + shift(c, kc_, 2), pl.ds(soon, late), :]
        send(got, got, lsc_sem, (kc_,), core_peer).wait_recv()
    for bb in range(2):

        @pl.when(bb != far)
        def _():
            for cc in range(2):
                for j in range(n_ch):
                    emit(bb, cc, j, 1)

    for n, step in enumerate(steps):
        if n:
            peer = moved(step)
            start(send(mg.at[lax.div(place_of(peer), n_u)], mgx.at[n], mg_sem, (n,), peer))

    block = lax.div(place_of(at()), n_u)
    total = ga[block].astype(F32)
    for n in range(1, n_dp):
        send(ga.at[0], gax.at[n], ga_sem, (n,), core_peer).wait_recv()
        total = total + gax[n].astype(F32)
    share = cols // n_u
    for q in range(n_u):

        @pl.when(lax.rem(place_of(at()), n_u) == q)
        def _():
            ga_out[...] = total[:, q * share : (q + 1) * share]

    total = gb[:, lanes_of(at())]
    for n in range(1, len(groups)):
        send(gbx.at[0], gbx.at[n], gb_sem, (n,), core_peer).wait_recv()
        total = total + gbx[n]
    for q in range(size_b // share_b):

        @pl.when(lax.rem(place_of(at()), size_b // share_b) == q)
        def _():
            gb_out[...] = total[:, q * share_b : (q + 1) * share_b]

    for place in range(2):
        for keep, copy in waiting[place]:

            @pl.when(jnp.logical_not(keep))
            def _():
                copy().wait_send()

    @pl.when(u == t)
    def _():
        for n, step in enumerate(steps):
            if n:
                for copy in packet(n, step):
                    copy.wait_send()

    for k in range(1, n_u):
        for p in range(n_pc):
            wa(k, p).wait_send()
            got = w_rows(shift(u, n_u - k, n_u), x, p)
            for m in range(1, n_x):
                send(got, got, wr_sem, (k - 1, m - 1, p), x_to[m]).wait_send()
    for i in range(H_CHUNK, n_h):
        late_h(i).wait_send()
    late_part(shift(t, n_u - 1, n_u)).wait_send()
    for kc_ in range(2):
        late_scatter(kc_).wait_send()
    for kb in range(2):
        for kc_ in range(2):
            if kb or kc_:
                for j in range(n_ch):
                    scatter(kb, kc_, j).wait_send()
    for copy in sent:
        copy.wait_send()

    total = mg[block]
    for n in range(1, n_dp):
        send(mg.at[0], mgx.at[n], mg_sem, (n,), core_peer).wait_recv()
        total = total + mgx[n]
    total = total / jnp.sqrt(pk_s[block] + 1e-06)
    for q in range(n_u):

        @pl.when(lax.rem(place_of(at()), n_u) == q)
        def _():
            mag_out[...] = total[:, q * share : (q + 1) * share]


def fused(hidden, weight_t, factor_bt, factor_a, magnitude, cotangent, n_u, n_x):
    rows, depth = hidden.shape
    cols = weight_t.shape[0]
    rank = factor_a.shape[0]
    n_blk = 4 * n_x
    n_dp = n_blk * n_u
    n_ch, n_pc = len(chunks_of(cols, n_x)), len(pieces_of(cols, n_x))
    wide = n_x * LANES
    full = padded(n_x * cols)
    late = rows // LATE_SHARE
    n_h = H_CHUNK + LATE_CHUNK
    size_b = granule(depth, n_dp)
    groups = n_u * n_x
    few = max(n_x - 1, 1)
    sem = pltpu.SemaphoreType.DMA
    vmem = pltpu.VMEM
    whole = pl.BlockSpec(memory_space=pltpu.VMEM)
    return pl.pallas_call(
        functools.partial(kernel, n_u, n_x),
        out_shape=(
            jax.ShapeDtypeStruct(cotangent.shape, BF16),
            jax.ShapeDtypeStruct((1, cols // n_u), F32),
            jax.ShapeDtypeStruct((rank, cols // n_u), F32),
            jax.ShapeDtypeStruct((rank, depth // n_dp), F32),
        ),
        in_specs=[pl.BlockSpec(memory_space=pltpu.HBM)] * 2 + [whole] * 4,
        out_specs=(whole,) * 4,
        scratch_shapes=[
            vmem((4 * rows, depth), BF16),
            vmem((n_u, n_x, cols, depth), BF16),
            vmem((2, 4 * rows - 2 * late, wide), F32),
            vmem((2, 4 * rows - 2 * late, wide), BF16),
            vmem((n_u - 1, 4 * rows - 2 * late, full), BF16),
            vmem((4, rows, full), BF16),
            vmem((n_x * cols, 2 * late), F32),
            vmem((2 * late, full), F32),
            vmem((2 * late, full), BF16),
            vmem((n_u - 1, 2 * late, full), BF16),
            vmem((4, rows, full), BF16),
            vmem((8, cols), F32),
            vmem((n_u - 1, 8, cols), F32),
            vmem((rank, rows), F32),
            vmem((n_u - 1, rank, rows), F32),
            vmem((rank, rows), F32),
            vmem((n_u - 1, rank, rows), F32),
            vmem((4, rank, rows), BF16),
            vmem((n_blk, rank, cols), BF16),
            vmem((n_blk, 1, cols), F32),
            vmem((1, cols), F32),
            vmem((n_blk, rank, cols), BF16),
            vmem((n_dp, rank, cols), BF16),
            vmem((rank, depth), F32),
            vmem((groups, rank, size_b), F32),
            vmem((n_blk, 1, cols), F32),
            vmem((n_dp, 1, cols), F32),
            sem((3,)),
            sem((2, 2)),
            sem((2, n_h)),
            sem((2, n_h)),
            sem((2, few, n_pc)),
            sem((2, n_u - 1, n_pc)),
            sem((2, n_u - 1, few, n_pc)),
            sem((2,)),
            sem((2, n_ch, n_u - 1)),
            sem((2, 4, n_ch)),
            sem((1,)),
            sem((n_u - 1,)),
            sem((2, 2)),
            pltpu.SemaphoreType.REGULAR,
            sem((2, n_u - 1)),
            sem((2, n_u - 1)),
            sem((2, n_u - 1)),
            sem((2, 3)),
            sem((2, n_dp)),
            sem((2, n_blk)),
            sem((2, n_dp)),
            sem((2, groups)),
            sem((2, n_dp)),
        ],
        compiler_params=pltpu.CompilerParams(
            collective_id=0, has_side_effects=True, vmem_limit_bytes=67043328
        ),
        name="fused",
    )(hidden, weight_t, factor_bt, factor_a, magnitude, cotangent)


def body(hidden, weight, factor_b, factor_a, magnitude, cotangent, *, n_u, n_x):
    mixed, mag, ga, gb = fused(
        hidden, weight.T, factor_b.T, factor_a, magnitude[None], cotangent, n_u, n_x
    )
    return mixed, mag[0], ga, gb.T


def solution(mesh):
    n_dp, n_u = mesh.shape["dp"], mesh.shape["tensor"]
    n_x = n_dp // (4 * n_u)
    fine = Mesh(mesh.devices.reshape(n_u, 2, n_x, 2, n_u), AXES)
    dp = ("u", "b", "x", "core")

    def step(*args):
        return body(*args, n_u=n_u, n_x=n_x)

    return jax.shard_map(
        step,
        mesh=fine,
        in_specs=(
            P(dp, "tensor"),
            P("tensor", dp),
            P("tensor", None),
            P(None, dp),
            P("tensor"),
            P(dp, "tensor"),
        ),
        out_specs=(
            P(dp, "tensor"),
            P(("tensor",) + dp),
            P(None, ("tensor",) + dp),
            P(("tensor",) + dp, None),
        ),
        check_vma=False,
    )
```

```python
import functools

import jax
import jax.numpy as jnp
from jax import lax
from jax.experimental import pallas as pl
from jax.experimental.pallas import tpu as pltpu
from jax.sharding import Mesh, PartitionSpec as P

F32, BF16 = jnp.float32, jnp.bfloat16
AXES = ("u", "b", "x", "core", "tensor")
MESH = pl.DeviceIdType.MESH
NT = (((1,), (1,)), ((), ()))
NN = (((1,), (0,)), ((), ()))
TN = (((0,), (0,)), ((), ()))
H_PIECE = 48
LATE_SHARE = 20
PIECE = 16
LANES = 128


def split_of(size, most):
    best = LANES
    for step in range(LANES, most + 1, LANES):
        if size % step == 0:
            best = step
    return best


def cuts(size, step):
    return [(at, min(step, size - at)) for at in range(0, size, step)]


def chunks_of(cols, n_x):
    last = LANES // n_x
    rest = cols - LANES
    if rest <= last:
        return [(0, LANES), (LANES, rest)]
    return [(0, LANES), (LANES, rest - last), (cols - last, last)]


def granule(depth, n_dp):
    share = depth // n_dp
    size = share
    while size % LANES:
        size += share
    return size


def padded(lanes):
    return -(-lanes // LANES) * LANES


def dot(left, right, dims):
    return lax.dot_general(left, right, dims, preferred_element_type=F32)


def kernel(
    n_u, n_x, h, w, bt, a, mag, cot, mixed, mag_out, ga_out, gb_out,
    hs, ws, own, part_out, part_in, scat, late_sum, late_own, late_out, late_in, got_out, sq, sqx, low, lowx, back, backx, backs, pk_a, pk_s, pks,
    ga, gax, gb, gbx, mg, mgx,
    loc_sem, hc_sem, hb_sem, hr_sem, wx_sem, wa_sem, wr_sem, ps_sem, pr_sem, sc_sem, ls_sem, lr_sem, lsc_sem, turn_sem,
    sq_sem, low_sem, back_sem, tok_sem, pk_ssem, pk_rsem, ga_sem, gb_sem, mg_sem,
):
    u, b, x, c, t = (lax.axis_index(name) for name in AXES)
    rows, depth = h.shape
    cols = w.shape[0]
    rank = a.shape[0]
    n_blk = 4 * n_x
    n_dp = n_blk * n_u
    late = rows // LATE_SHARE
    soon = rows - late
    kc = split_of(depth, 1152)
    h_cuts = cuts(soon, H_PIECE) + [(soon, late)]
    n_h = len(h_cuts)
    n_soon = n_h - 1
    chunks = chunks_of(cols, n_x)
    pieces = cuts(cols, PIECE)
    n_ch, n_pc = len(chunks), len(pieces)
    lane_at = [sum(padded(n_x * size) for _, size in chunks[:j]) for j in range(n_ch)]

    def at(**moved):
        here = dict(u=u, b=b, x=x, core=c, tensor=t)
        here.update(moved)
        return tuple(here[name] for name in AXES)

    def shift(value, by, n):
        return lax.rem(value + by, n)

    def remote(src, dst, send_sem, recv_sem, peer):
        return pltpu.make_async_remote_copy(
            src_ref=src, dst_ref=dst, send_sem=send_sem, recv_sem=recv_sem, device_id=peer, device_id_type=MESH
        )

    def send(src, dst, sems, index, peer):
        return remote(src, dst, sems.at[(0,) + index], sems.at[(1,) + index], peer)

    core_peer = at(core=1 - c)
    b_peer = at(b=1 - b)
    x_to = [at(x=shift(x, k, n_x)) for k in range(n_x)]
    u_to = [at(u=shift(u, k, n_u), b=shift(b, k % 2, 2)) for k in range(n_u)]
    t_to = [at(tensor=shift(t, k, n_u)) for k in range(n_u)]
    steps = [(i, j, k, l) for i in range(n_u) for j in range(2) for k in range(n_x) for l in range(2)]

    def moved(step):
        du, db, dx, dc = step
        return at(u=shift(u, du, n_u), b=shift(b, db, 2), x=shift(x, dx, n_x), core=shift(c, dc, 2))

    def place_of(device):
        return ((device[0] * 2 + device[1]) * n_x + device[2]) * 2 + device[3]

    def block_of(bb, xx, cc):
        return (bb * n_x + xx) * 2 + cc

    far = shift(b, u - t + n_u, 2)

    peers = [moved(step) for step in steps[1:]] + t_to[1:]
    barrier = pltpu.get_barrier_semaphore()
    for peer in peers:
        pl.semaphore_signal(barrier, inc=1, device_id=peer, device_id_type=MESH)
    pl.semaphore_wait(barrier, len(peers))

    def row_of(kb, cc, first):
        return kb * 2 * rows + (cc * soon + first if first < soon else 2 * soon + cc * late + first - soon)

    def rows_at(kb, cc, first, size):
        return pl.ds(pl.multiple_of(row_of(kb, cc, first), 16), size)

    halves = [(0, soon), (soon, late)]

    def h_rows(kb, cc, i):
        return hs.at[rows_at(kb, cc, *h_cuts[i]), :]

    def w_rows(uu, xx, p):
        first, size = pieces[p]
        return ws.at[uu, xx, pl.ds(first, size), :]

    def half_rows(cc, half):
        return hs.at[rows_at(0, cc, *halves[half]), :]

    sent = []

    def start(copy):
        copy.start()
        sent.append(copy)

    def late_h(i):
        return send(h.at[pl.ds(*h_cuts[i]), :], h_rows(1, c, i), hb_sem, (i,), b_peer)

    def start_h(i):
        start(late_h(i))

    def start_wx(p):
        first, size = pieces[p]
        for k in range(1, n_x):
            start(send(w.at[pl.ds(first, size), :], w_rows(u, x, p), wx_sem, (k - 1, p), x_to[k]))

    def wa(k, p):
        first, size = pieces[p]
        return send(w.at[pl.ds(first, size), :], w_rows(u, x, p), wa_sem, (k - 1, p), u_to[k])

    def start_wa(p):
        for k in range(1, n_u):
            wa(k, p).start()

    early = lax.rem(u, 2) != b

    loads = [
        pltpu.make_async_copy(w, ws.at[u, x], loc_sem.at[1]),
    ] + [
        pltpu.make_async_copy(h.at[pl.ds(*halves[i]), :], half_rows(c, i), loc_sem.at[2 * i]) for i in range(2)
    ]
    for load in loads:
        load.start()
    for i in range(2):
        start(send(h.at[pl.ds(*halves[i]), :], half_rows(c, i), hc_sem, (i,), core_peer))
    start_h(0)
    for p in range(4):
        start_wx(p)

    @pl.when(early)
    def _():
        for p in range(4):
            start_wa(p)

    loads[0].wait()
    a_t = jnp.transpose(a[...].astype(F32)).astype(BF16)

    def square_step(i, acc):
        at_k = pl.ds(pl.multiple_of(i * kc, LANES), kc)
        merged = ws[u, x, :, at_k].astype(F32) + dot(a_t, bt[:, at_k], NN)
        for g in range(kc // LANES):
            part = merged[:, g * LANES : (g + 1) * LANES]
            acc = acc + part * part
        return acc

    squares = lax.fori_loop(0, depth // kc, square_step, jnp.zeros((cols, LANES), F32))
    sq[...] = lax.dot_general(
        jnp.ones((8, LANES), F32), squares, NT, precision=lax.Precision.HIGHEST, preferred_element_type=F32
    )
    for k in range(1, n_u):
        start(send(sq, sqx.at[k - 1], sq_sem, (k - 1,), t_to[k]))

    loads[1].wait()
    loads[2].wait()

    def low_step(i, acc):
        at_k = pl.ds(pl.multiple_of(i * kc, LANES), kc)
        left = jnp.concatenate([hs[rows_at(0, c, *half), at_k] for half in halves], axis=0)
        return acc + dot(bt[:, at_k], left, NT)

    low[...] = lax.fori_loop(0, depth // kc, low_step, jnp.zeros((rank, rows), F32))
    for k in range(1, n_u):
        start(send(low, lowx.at[k - 1], low_sem, (k - 1,), t_to[k]))

    def from_t(ref, extra, sems):
        total = ref[...]
        for k in range(1, n_u):
            send(ref, extra.at[k - 1], sems, (k - 1,), t_to[k]).wait_recv()
            total = total + extra[k - 1]
        return total

    square_sum = from_t(sq, sqx, sq_sem)
    mine = block_of(b, x, c)

    def packet(n, step):
        return [
            remote(a, pk_a.at[mine], pk_ssem.at[0, n], pk_rsem.at[0, n % n_blk], moved(step)),
            remote(pks, pk_s.at[mine], pk_ssem.at[1, n], pk_rsem.at[1, n % n_blk], moved(step)),
        ]

    @pl.when(u == t)
    def _():
        pks[...] = square_sum[0:1, :]
        pk_a[mine] = a[...]
        pk_s[mine] = square_sum[0:1, :]
        for n, step in enumerate(steps):
            if n:
                for copy in packet(n, step):
                    copy.start()

    for i in range(1, 3):
        start_h(i)
    for p in range(4, 8):
        start_wx(p)

    @pl.when(early)
    def _():
        for p in range(4, 8):
            start_wa(p)

    low_t = from_t(low, lowx, low_sem)
    low_tb = low_t.astype(BF16)
    low_b = jnp.transpose(low_t).astype(BF16)

    count = [0]
    waiting = [[], []]

    def lag_of(uu):
        return lax.rem(uu - t + 2 * n_u - 1, n_u)

    def lanes_in(j):
        first, size = chunks[j]
        return pl.ds(lane_at[j], padded(n_x * size))

    spans = {0: (0, 2 * rows), 1: (2 * rows, 2 * soon), 2: (0, 2 * (rows + soon))}

    def run_unit(kb, ku, j):
        first, size = chunks[j]
        wide = n_x * size
        top, tall = spans[kb]
        place = count[0] % 2
        count[0] += 1
        uu = shift(u, ku, n_u)
        keep = uu == t

        def copy():
            return remote(
                part_out.at[place, 0:tall, 0 : padded(wide)], part_in.at[lag_of(uu), top : top + tall, lanes_in(j)],
                ps_sem.at[place], pr_sem.at[min(kb, 1), j, lag_of(uu)], at(tensor=uu),
            )

        if waiting[place]:
            old_keep, old_copy = waiting[place].pop()

            @pl.when(jnp.logical_not(old_keep))
            def _():
                old_copy().wait_send()

        own[place, 0:tall, 0:wide] = jnp.zeros((tall, wide), F32)

        def unit_step(i, carry):
            at_k = pl.ds(pl.multiple_of(i * kc, LANES), kc)
            right = jnp.concatenate([ws[uu, xx, first : first + size, at_k] for xx in range(n_x)], axis=0)
            own[place, 0:tall, 0:wide] += dot(hs[top : top + tall, at_k], right, NT)
            return carry

        lax.fori_loop(0, depth // kc, unit_step, 0)

        @pl.when(jnp.logical_not(keep))
        def _():
            part_out[place, 0:tall, 0:wide] = own[place, 0:tall, 0:wide].astype(BF16)
            copy().start()

        waiting[place].append((keep, copy))
        return kb, uu, j, place

    def scatter(kb, kc_, j):
        index = (kb * 2 + kc_, j)
        span = pl.ds(0, soon if kb else rows)
        return send(
            scat.at[kb * 2 + kc_, span, lanes_in(j)], got_out.at[far * 2 + c, span, lanes_in(j)], sc_sem, index,
            at(b=shift(b, kb, 2), core=shift(c, kc_, 2)),
        )

    def finish(kb, uu, j, place):
        first, size = chunks[j]
        wide = n_x * size
        top, tall = spans[kb]
        lanes = pl.ds(lane_at[j], wide)

        @pl.when(uu == t)
        def _():
            for k in range(n_u - 1):
                remote(
                    part_out.at[0, 0:tall, 0 : padded(wide)], part_in.at[k, top : top + tall, lanes_in(j)],
                    ps_sem.at[0], pr_sem.at[min(kb, 1), j, k], t_to[1],
                ).wait_recv()
            for side in (0, 1) if kb == 2 else (kb,):
                for kc_ in range(2):
                    for half in halves[: 1 if side else 2]:
                        at_c = row_of(side, shift(c, kc_, 2), half[0])
                        total = own[place, pl.ds(pl.multiple_of(at_c - top, 16), half[1]), 0:wide]
                        for k in range(n_u - 1):
                            more = part_in[k, pl.ds(pl.multiple_of(at_c, 16), half[1]), lanes]
                            total = total + more.astype(F32)
                        if side == 0 and kc_ == 0:
                            got_out[far * 2 + c, pl.ds(*half), lanes] = total.astype(BF16)
                        else:
                            scat[side * 2 + kc_, pl.ds(*half), lanes] = total.astype(BF16)
                    if side and deferred:
                        deferred[0].append((uu, side, kc_, j))
                    elif side or kc_:
                        scatter(side, kc_, j).start()

    pending, deferred = [], [[]]

    def go(kb, ku, j):
        new = run_unit(kb, ku, j)
        if pending:
            finish(*pending.pop())
        pending.append(new)

    def late_part(uu):
        return remote(late_out, late_in.at[lag_of(uu)], ls_sem.at[0], lr_sem.at[lag_of(uu)], at(tensor=uu))

    def late_unit(uu):
        late_sum[...] = jnp.zeros(late_sum.shape, F32)

        def late_step(i, carry):
            at_k = pl.ds(pl.multiple_of(i * kc, LANES), kc)
            right = jnp.concatenate(
                [ws[uu, xx, first : first + size, at_k] for first, size in chunks for xx in range(n_x)], axis=0
            )
            late_sum[...] += dot(right, hs[2 * (rows + soon) : 4 * rows, at_k], NT)
            return carry

        lax.fori_loop(0, depth // kc, late_step, 0)
        flat = jnp.transpose(late_sum[...])
        return [(lane_at[j], flat[:, n_x * at : n_x * (at + size)]) for j, (at, size) in enumerate(chunks)]

    def late_scatter(kc_):
        return send(
            scat.at[2 + kc_, pl.ds(soon, late), :], got_out.at[far * 2 + c, pl.ds(soon, late), :], lsc_sem, (kc_,),
            at(b=1 - b, core=shift(c, kc_, 2)),
        )

    passed = [0]

    def pass_h():
        i = passed[0]
        passed[0] += 1
        got = h_rows(1, c, i)
        send(got, got, hb_sem, (i,), b_peer).wait_recv()
        start(send(got, got, hr_sem, (i,), core_peer))

    def near(p):
        for k in range(1, n_x):
            got = w_rows(u, shift(x, n_x - k, n_x), p)
            send(got, got, wx_sem, (k - 1, p), x_to[k]).wait_recv()

    def of_chunk(j):
        first, size = chunks[j]
        return [p for p in range(n_pc) if first <= pieces[p][0] < first + size]

    for q in range(n_blk):
        _, db, dx, dc = steps[q]
        src = block_of(shift(b, db, 2), shift(x, n_x - dx, n_x), shift(c, dc, 2))
        for wait in (
            remote(a, pk_a.at[src], pk_ssem.at[0, 0], pk_rsem.at[0, q], core_peer),
            remote(pks, pk_s.at[src], pk_ssem.at[1, 0], pk_rsem.at[1, q], core_peer),
        ):
            if q:
                wait.wait_recv()
            else:
                pl.when(u != t)(wait.wait_recv)

    def scale_of(i, first, size):
        norm = jnp.sqrt(pk_s[i, 0:1, first : first + size] + 1e-06)
        return mag[:, i * cols + first : i * cols + first + size] / norm

    back_part = jnp.zeros((rank, rows), F32)
    for i in range(n_blk):
        piece = cot[:, i * cols : (i + 1) * cols].astype(F32)
        dpre = (piece * scale_of(i, 0, cols)).astype(BF16)
        back_part = back_part + dot(pk_a[i], dpre, NT)
        ga[i] = dot(low_tb, dpre, NN).astype(BF16)
    back[...] = back_part
    for k in range(1, n_u):
        start(send(back, backx.at[k - 1], back_sem, (k - 1,), t_to[k]))
    back_b = from_t(back, backx, back_sem).astype(BF16)
    backs[c] = back_b
    for k in range(1, 4):
        peer = at(b=shift(b, k // 2, 2), core=shift(c, k % 2, 2))
        start(send(backs.at[c], backs.at[k // 2 * 2 + c], tok_sem, (k - 1,), peer))

    for i in range(3, n_soon):
        start_h(i)
    for p in range(8, n_pc):
        start_wx(p)

    @pl.when(early)
    def _():
        for p in range(8, n_pc):
            start_wa(p)

    for i in range(2):
        send(half_rows(1 - c, i), half_rows(1 - c, i), hc_sem, (i,), core_peer).wait_recv()

    def turn(peer):
        pl.semaphore_signal(turn_sem, inc=1, device_id=peer, device_id_type=MESH)

    def w_arrived(k, p):
        got = w_rows(shift(u, n_u - k, n_u), x, p)
        send(got, got, wa_sem, (k - 1, p), u_to[k]).wait_recv()
        for m in range(1, n_x):
            send(got, got, wr_sem, (k - 1, m - 1, p), x_to[m]).start()

    for j in range(n_ch):
        while passed[0] < n_soon * (j + 1) // n_ch:
            pass_h()
        for p in of_chunk(j):
            near(p)
        if j >= n_ch - 2:

            @pl.when(early)
            def _():
                for k in range(1, n_u):
                    for p in range(n_pc):
                        if (p in of_chunk(n_ch - 1)) == (j == n_ch - 1):
                            w_arrived(k, p)
                if j == n_ch - 1:
                    turn(at(u=shift(u, 1, n_u)))

        if j == n_ch - 1:

            @pl.when(jnp.logical_not(early))
            def _():
                pl.semaphore_wait(turn_sem, 1)
                for p in range(n_pc):
                    start_wa(p)
                for i in range(n_soon, n_h):
                    late_h(i).start()

        go(0, 0, j)
    for i in range(n_soon):
        got = h_rows(1, 1 - c, i)
        send(got, got, hr_sem, (i,), core_peer).wait_recv()

    for n, step in enumerate(steps):
        if n:
            peer = moved(step)
            start(send(ga.at[lax.div(place_of(peer), n_u)], gax.at[n], ga_sem, (n,), peer))

    for k in range(1, 4):
        src = k // 2 * 2 + shift(c, k % 2, 2)
        send(backs.at[src], backs.at[src], tok_sem, (k - 1,), core_peer).wait_recv()

    def grad_of(kb, half, at_k):
        first, size = halves[half]
        total = jnp.zeros((rank, kc), F32)
        for cc in range(2):
            held = hs[row_of(kb, cc, first) : row_of(kb, cc, first) + size, at_k]
            total = total + dot(backs[kb * 2 + cc, :, first : first + size], held, NN)
        return total

    def grad_step(i, carry):
        at_k = pl.ds(pl.multiple_of(i * kc, LANES), kc)
        total = jnp.zeros((rank, kc), F32)
        for kb, half in ((0, 0), (0, 1), (1, 0)):
            total = total + grad_of(kb, half, at_k)
        gb[:, at_k] = total
        return carry

    lax.fori_loop(0, depth // kc, grad_step, 0)
    size_b = granule(depth, n_dp)
    share_b = depth // n_dp

    def lanes_of(device):
        return pl.ds(pl.multiple_of(lax.div(place_of(device) * share_b, size_b) * size_b, LANES), size_b)

    groups = [step for step in steps if step[1] == 0 and step[3] == 0]
    def emit(bb, cc, j, half):
        first, size = chunks[j]
        span = pl.ds(*halves[half])
        for xx in range(n_x):
            i = block_of(bb, xx, cc)
            left = i * cols + first
            lane = lane_at[j] + xx * size
            pre = got_out[bb * 2 + cc, span, lane : lane + size].astype(F32)
            low_half = low_b[halves[half][0] : sum(halves[half]), :]
            pre = pre + dot(low_half, pk_a[i, :, first : first + size], NN)
            mixed[span, left : left + size] = (pre * scale_of(i, first, size)).astype(BF16)
            part = jnp.sum(cot[span, left : left + size].astype(F32) * pre, axis=0, keepdims=True)
            if half:
                mg[i, 0:1, first : first + size] += part
            else:
                mg[i, 0:1, first : first + size] = part

    def scattered(bb, cc, j, span):
        kind = lax.rem(bb + far, 2) * 2 + lax.rem(cc + c, 2)
        got = got_out.at[bb * 2 + cc, span, lanes_in(j)]
        return send(got, got, sc_sem, (kind, j), core_peer)

    def near_outputs(which):
        for bb in range(2):

            @pl.when(bb == far)
            def _():
                for j in which:
                    for cc in range(2):
                        pl.when(cc != c)(scattered(bb, cc, j, pl.ds(0, rows)).wait_recv)
                        for half in range(2):
                            emit(bb, cc, j, half)

    def far_outputs(which, half):
        for bb in range(2):

            @pl.when(bb != far)
            def _():
                for j in which:
                    for cc in range(2):
                        if half == 0:
                            scattered(bb, cc, j, pl.ds(0, soon)).wait_recv()
                        emit(bb, cc, j, half)

    def far_piece(k, p):
        @pl.when(jnp.logical_not(early))
        def _():
            w_arrived(k, p)
            if k == n_u - 1 and p == n_pc - 1:
                turn(b_peer)

    def far_ready(k, j):
        for p in of_chunk(j):
            for m in range(1, n_x):
                got = w_rows(shift(u, n_u - k, n_u), shift(x, n_x - m, n_x), p)
                send(got, got, wr_sem, (k - 1, m - 1, p), x_to[m]).wait_recv()

    units = [(1, 0, j) for j in range(n_ch)]
    early_out = 2 if n_ch > 2 else 0

    for k in range(1, n_u):
        for p in range(n_pc):
            if pending:
                finish(*pending.pop())
            elif units:
                pending.append(run_unit(*units.pop(0)))
            if k == n_u - 1 and n_ch > 2 and p == n_pc - 5:
                near_outputs([0])
            far_piece(k, p)
            for j in range(n_ch - 1):
                if max(of_chunk(j)) + 2 == p:
                    far_ready(k, j)
                    units += [(0, n_u - k, j), (1, n_u - k, j)]
        if k == n_u - 1:

            @pl.when(early)
            def _():
                pl.semaphore_wait(turn_sem, 1)
                late_h(n_soon).start()

        while units:
            go(*units.pop(0))
        if k == n_u - 1:
            near_outputs(range(max(early_out - 1, 0), early_out))
        for j in range(n_ch):
            if max(of_chunk(j)) + 2 >= n_pc:
                far_ready(k, j)
                if k == n_u - 1 and deferred:
                    for uu, side, kc_, i in deferred.pop():
                        pl.when(uu == t)(scatter(side, kc_, i).start)
                go(2, n_u - k, j)

    for i in range(n_soon, n_h):
        pass_h()
    for i in range(n_soon, n_h):
        got = h_rows(1, 1 - c, i)
        send(got, got, hr_sem, (i,), core_peer).wait_recv()
    for k in range(1, n_u):
        if k > 1:
            late_part(shift(t, k - 1, n_u)).wait_send()
        for lane, part in late_unit(shift(t, k, n_u)):
            late_out[:, lane : lane + part.shape[1]] = part.astype(BF16)
        late_part(shift(t, k, n_u)).start()
    finish(*pending.pop())

    def grad_late(i, carry):
        at_k = pl.ds(pl.multiple_of(i * kc, LANES), kc)
        gb[:, at_k] += grad_of(1, 1, at_k)
        return carry

    lax.fori_loop(0, depth // kc, grad_late, 0)
    for n, step in enumerate(groups):
        if n:
            peer = moved(step)
            start(send(gb.at[:, lanes_of(peer)], gbx.at[n], gb_sem, (n,), peer))
    for lane, part in late_unit(t):
        late_own[:, lane : lane + part.shape[1]] = part

    for k in range(n_u - 1):
        remote(late_out, late_in.at[k], ls_sem.at[0], lr_sem.at[k], t_to[1]).wait_recv()
    for kc_ in range(2):
        at_c = pl.ds(pl.multiple_of(shift(c, kc_, 2) * late, 16), late)
        for j, (_, size) in enumerate(chunks):
            lanes = pl.ds(lane_at[j], n_x * size)
            total = late_own[at_c, lanes]
            for k in range(n_u - 1):
                total = total + late_in[k, at_c, lanes].astype(F32)
            scat[2 + kc_, pl.ds(soon, late), lanes] = total.astype(BF16)
        late_scatter(kc_).start()
    near_outputs(range(early_out, n_ch))
    far_outputs(range(n_ch), 0)
    for kc_ in range(2):
        got = got_out.at[(1 - far) * 2 + shift(c, kc_, 2), pl.ds(soon, late), :]
        send(got, got, lsc_sem, (kc_,), core_peer).wait_recv()
    far_outputs(range(n_ch), 1)

    for n, step in enumerate(steps):
        if n:
            peer = moved(step)
            start(send(mg.at[lax.div(place_of(peer), n_u)], mgx.at[n], mg_sem, (n,), peer))

    block = lax.div(place_of(at()), n_u)
    total = ga[block].astype(F32)
    for n in range(1, n_dp):
        send(ga.at[0], gax.at[n], ga_sem, (n,), core_peer).wait_recv()
        total = total + gax[n].astype(F32)
    share = cols // n_u
    for q in range(n_u):

        @pl.when(lax.rem(place_of(at()), n_u) == q)
        def _():
            ga_out[...] = total[:, q * share : (q + 1) * share]

    total = gb[:, lanes_of(at())]
    for n in range(1, len(groups)):
        send(gbx.at[0], gbx.at[n], gb_sem, (n,), core_peer).wait_recv()
        total = total + gbx[n]
    for q in range(size_b // share_b):

        @pl.when(lax.rem(place_of(at()), size_b // share_b) == q)
        def _():
            gb_out[...] = total[:, q * share_b : (q + 1) * share_b]

    for place in range(2):
        for keep, copy in waiting[place]:

            @pl.when(jnp.logical_not(keep))
            def _():
                copy().wait_send()

    @pl.when(u == t)
    def _():
        for n, step in enumerate(steps):
            if n:
                for copy in packet(n, step):
                    copy.wait_send()

    for k in range(1, n_u):
        for p in range(n_pc):
            wa(k, p).wait_send()
            got = w_rows(shift(u, n_u - k, n_u), x, p)
            for m in range(1, n_x):
                send(got, got, wr_sem, (k - 1, m - 1, p), x_to[m]).wait_send()
    for i in range(n_soon, n_h):
        late_h(i).wait_send()
    late_part(shift(t, n_u - 1, n_u)).wait_send()
    for kc_ in range(2):
        late_scatter(kc_).wait_send()
    for kb in range(2):
        for kc_ in range(2):
            if kb or kc_:
                for j in range(n_ch):
                    scatter(kb, kc_, j).wait_send()
    for copy in sent:
        copy.wait_send()

    total = mg[block]
    for n in range(1, n_dp):
        send(mg.at[0], mgx.at[n], mg_sem, (n,), core_peer).wait_recv()
        total = total + mgx[n]
    total = total / jnp.sqrt(pk_s[block] + 1e-06)
    for q in range(n_u):

        @pl.when(lax.rem(place_of(at()), n_u) == q)
        def _():
            mag_out[...] = total[:, q * share : (q + 1) * share]


def fused(hidden, weight_t, factor_bt, factor_a, magnitude, cotangent, n_u, n_x):
    rows, depth = hidden.shape
    cols = weight_t.shape[0]
    rank = factor_a.shape[0]
    n_blk = 4 * n_x
    n_dp = n_blk * n_u
    n_ch, n_pc = len(chunks_of(cols, n_x)), len(cuts(cols, PIECE))
    wide = n_x * LANES
    full = sum(padded(n_x * size) for _, size in chunks_of(cols, n_x))
    late = rows // LATE_SHARE
    n_h = len(cuts(rows - late, H_PIECE)) + 1
    size_b = granule(depth, n_dp)
    groups = n_u * n_x
    few = max(n_x - 1, 1)
    sem = pltpu.SemaphoreType.DMA
    vmem = pltpu.VMEM
    whole = pl.BlockSpec(memory_space=pltpu.VMEM)
    return pl.pallas_call(
        functools.partial(kernel, n_u, n_x),
        out_shape=(
            jax.ShapeDtypeStruct(cotangent.shape, BF16),
            jax.ShapeDtypeStruct((1, cols // n_u), F32),
            jax.ShapeDtypeStruct((rank, cols // n_u), F32),
            jax.ShapeDtypeStruct((rank, depth // n_dp), F32),
        ),
        in_specs=[pl.BlockSpec(memory_space=pltpu.HBM)] * 2 + [whole] * 4,
        out_specs=(whole,) * 4,
        scratch_shapes=[
            vmem((4 * rows, depth), BF16),
            vmem((n_u, n_x, cols, depth), BF16),
            vmem((2, 4 * rows - 2 * late, wide), F32),
            vmem((2, 4 * rows - 2 * late, wide), BF16),
            vmem((n_u - 1, 4 * rows - 2 * late, full), BF16),
            vmem((4, rows, full), BF16),
            vmem((n_x * cols, 2 * late), F32),
            vmem((2 * late, full), F32),
            vmem((2 * late, full), BF16),
            vmem((n_u - 1, 2 * late, full), BF16),
            vmem((4, rows, full), BF16),
            vmem((8, cols), F32),
            vmem((n_u - 1, 8, cols), F32),
            vmem((rank, rows), F32),
            vmem((n_u - 1, rank, rows), F32),
            vmem((rank, rows), F32),
            vmem((n_u - 1, rank, rows), F32),
            vmem((4, rank, rows), BF16),
            vmem((n_blk, rank, cols), BF16),
            vmem((n_blk, 1, cols), F32),
            vmem((1, cols), F32),
            vmem((n_blk, rank, cols), BF16),
            vmem((n_dp, rank, cols), BF16),
            vmem((rank, depth), F32),
            vmem((groups, rank, size_b), F32),
            vmem((n_blk, 1, cols), F32),
            vmem((n_dp, 1, cols), F32),
            sem((3,)),
            sem((2, 2)),
            sem((2, n_h)),
            sem((2, n_h)),
            sem((2, few, n_pc)),
            sem((2, n_u - 1, n_pc)),
            sem((2, n_u - 1, few, n_pc)),
            sem((2,)),
            sem((2, n_ch, n_u - 1)),
            sem((2, 4, n_ch)),
            sem((1,)),
            sem((n_u - 1,)),
            sem((2, 2)),
            pltpu.SemaphoreType.REGULAR,
            sem((2, n_u - 1)),
            sem((2, n_u - 1)),
            sem((2, n_u - 1)),
            sem((2, 3)),
            sem((2, n_dp)),
            sem((2, n_blk)),
            sem((2, n_dp)),
            sem((2, groups)),
            sem((2, n_dp)),
        ],
        compiler_params=pltpu.CompilerParams(
            collective_id=0, has_side_effects=True, vmem_limit_bytes=67043328
        ),
        name="fused",
    )(hidden, weight_t, factor_bt, factor_a, magnitude, cotangent)


def body(hidden, weight, factor_b, factor_a, magnitude, cotangent, *, n_u, n_x):
    mixed, mag, ga, gb = fused(
        hidden, weight.T, factor_b.T, factor_a, magnitude[None], cotangent, n_u, n_x
    )
    return mixed, mag[0], ga, gb.T


def solution(mesh):
    n_dp, n_u = mesh.shape["dp"], mesh.shape["tensor"]
    n_x = n_dp // (4 * n_u)
    fine = Mesh(mesh.devices.reshape(n_u, 2, n_x, 2, n_u), AXES)
    dp = ("u", "b", "x", "core")

    def step(*args):
        return body(*args, n_u=n_u, n_x=n_x)

    return jax.shard_map(
        step,
        mesh=fine,
        in_specs=(
            P(dp, "tensor"),
            P("tensor", dp),
            P("tensor", None),
            P(None, dp),
            P("tensor"),
            P(dp, "tensor"),
        ),
        out_specs=(
            P(dp, "tensor"),
            P(("tensor",) + dp),
            P(None, ("tensor",) + dp),
            P(("tensor",) + dp, None),
        ),
        check_vma=False,
    )
```

```python
import functools

import jax
import jax.numpy as jnp
from jax import lax
from jax.experimental import pallas as pl
from jax.experimental.pallas import tpu as pltpu
from jax.sharding import Mesh, PartitionSpec as P

F32, BF16 = jnp.float32, jnp.bfloat16
AXES = ("u", "b", "x", "core", "tensor")
MESH = pl.DeviceIdType.MESH
NT = (((1,), (1,)), ((), ()))
NN = (((1,), (0,)), ((), ()))
TN = (((0,), (0,)), ((), ()))
H_PIECE = 48
LATE_SHARE = 20
PIECE = 16
LANES = 128


def split_of(size, most):
    best = LANES
    for step in range(LANES, most + 1, LANES):
        if size % step == 0:
            best = step
    return best


def cuts(size, step):
    return [(at, min(step, size - at)) for at in range(0, size, step)]


def chunks_of(cols, n_x):
    last = LANES // n_x
    rest = cols - LANES
    if rest <= last:
        return [(0, LANES), (LANES, rest)]
    return [(0, LANES), (LANES, rest - last), (cols - last, last)]


def granule(depth, n_dp):
    share = depth // n_dp
    size = share
    while size % LANES:
        size += share
    return size


def padded(lanes):
    return -(-lanes // LANES) * LANES


def dot(left, right, dims):
    return lax.dot_general(left, right, dims, preferred_element_type=F32)


def kernel(
    n_u, n_x, h, w, bt, a, mag, cot, mixed, mag_out, ga_out, gb_out,
    hs, ws, own, part_out, part_in, scat, late_sum, late_own, late_out, late_in, got_out, sq, sqx, low, lowx, back, backx, backs, pk_a, pk_s, pks,
    ga, gax, gb, gbx, mg, mgx,
    loc_sem, hc_sem, hb_sem, hr_sem, wx_sem, wa_sem, wr_sem, ps_sem, pr_sem, sc_sem, ls_sem, lr_sem, lsc_sem, turn_sem,
    sq_sem, low_sem, back_sem, tok_sem, pk_ssem, pk_rsem, ga_sem, gb_sem, mg_sem,
):
    u, b, x, c, t = (lax.axis_index(name) for name in AXES)
    rows, depth = h.shape
    cols = w.shape[0]
    rank = a.shape[0]
    n_blk = 4 * n_x
    n_dp = n_blk * n_u
    late = rows // LATE_SHARE
    soon = rows - late
    kc = split_of(depth, 1152)
    k_step = split_of(depth, 4608)
    h_cuts = cuts(soon, H_PIECE) + [(soon, late)]
    n_h = len(h_cuts)
    n_soon = n_h - 1
    chunks = chunks_of(cols, n_x)
    pieces = cuts(cols, PIECE)
    n_ch, n_pc = len(chunks), len(pieces)
    lane_at = [sum(padded(n_x * size) for _, size in chunks[:j]) for j in range(n_ch)]

    def at(**moved):
        here = dict(u=u, b=b, x=x, core=c, tensor=t)
        here.update(moved)
        return tuple(here[name] for name in AXES)

    def shift(value, by, n):
        return lax.rem(value + by, n)

    def remote(src, dst, send_sem, recv_sem, peer):
        return pltpu.make_async_remote_copy(
            src_ref=src, dst_ref=dst, send_sem=send_sem, recv_sem=recv_sem, device_id=peer, device_id_type=MESH
        )

    def send(src, dst, sems, index, peer):
        return remote(src, dst, sems.at[(0,) + index], sems.at[(1,) + index], peer)

    core_peer = at(core=1 - c)
    b_peer = at(b=1 - b)
    x_to = [at(x=shift(x, k, n_x)) for k in range(n_x)]
    u_to = [at(u=shift(u, k, n_u), b=shift(b, k % 2, 2)) for k in range(n_u)]
    t_to = [at(tensor=shift(t, k, n_u)) for k in range(n_u)]
    steps = [(i, j, k, l) for i in range(n_u) for j in range(2) for k in range(n_x) for l in range(2)]

    def moved(step):
        du, db, dx, dc = step
        return at(u=shift(u, du, n_u), b=shift(b, db, 2), x=shift(x, dx, n_x), core=shift(c, dc, 2))

    def place_of(device):
        return ((device[0] * 2 + device[1]) * n_x + device[2]) * 2 + device[3]

    def block_of(bb, xx, cc):
        return (bb * n_x + xx) * 2 + cc

    far = shift(b, u - t + n_u, 2)

    peers = [moved(step) for step in steps[1:]] + t_to[1:]
    barrier = pltpu.get_barrier_semaphore()
    for peer in peers:
        pl.semaphore_signal(barrier, inc=1, device_id=peer, device_id_type=MESH)
    pl.semaphore_wait(barrier, len(peers))

    def row_of(kb, cc, first):
        return kb * 2 * rows + (cc * soon + first if first < soon else 2 * soon + cc * late + first - soon)

    def rows_at(kb, cc, first, size):
        return pl.ds(pl.multiple_of(row_of(kb, cc, first), 16), size)

    halves = [(0, soon), (soon, late)]

    def h_rows(kb, cc, i):
        return hs.at[rows_at(kb, cc, *h_cuts[i]), :]

    def w_rows(uu, xx, p):
        first, size = pieces[p]
        return ws.at[uu, xx, pl.ds(first, size), :]

    def half_rows(cc, half):
        return hs.at[rows_at(0, cc, *halves[half]), :]

    sent = []

    def start(copy):
        copy.start()
        sent.append(copy)

    def late_h(i):
        return send(h.at[pl.ds(*h_cuts[i]), :], h_rows(1, c, i), hb_sem, (i,), b_peer)

    def start_h(i):
        start(late_h(i))

    def start_wx(p):
        first, size = pieces[p]
        for k in range(1, n_x):
            start(send(w.at[pl.ds(first, size), :], w_rows(u, x, p), wx_sem, (k - 1, p), x_to[k]))

    def wa(k, p):
        first, size = pieces[p]
        return send(w.at[pl.ds(first, size), :], w_rows(u, x, p), wa_sem, (k - 1, p), u_to[k])

    def start_wa(p):
        for k in range(1, n_u):
            wa(k, p).start()

    early = lax.rem(u, 2) != b

    loads = [
        pltpu.make_async_copy(w, ws.at[u, x], loc_sem.at[1]),
    ] + [
        pltpu.make_async_copy(h.at[pl.ds(*halves[i]), :], half_rows(c, i), loc_sem.at[2 * i]) for i in range(2)
    ]
    for load in loads:
        load.start()
    for i in range(2):
        start(send(h.at[pl.ds(*halves[i]), :], half_rows(c, i), hc_sem, (i,), core_peer))
    start_h(0)
    for p in range(4):
        start_wx(p)

    @pl.when(early)
    def _():
        for p in range(4):
            start_wa(p)

    loads[0].wait()
    a_t = jnp.transpose(a[...].astype(F32)).astype(BF16)

    def square_step(i, acc):
        at_k = pl.ds(pl.multiple_of(i * kc, LANES), kc)
        merged = ws[u, x, :, at_k].astype(F32) + dot(a_t, bt[:, at_k], NN)
        for g in range(kc // LANES):
            part = merged[:, g * LANES : (g + 1) * LANES]
            acc = acc + part * part
        return acc

    squares = lax.fori_loop(0, depth // kc, square_step, jnp.zeros((cols, LANES), F32))
    sq[...] = lax.dot_general(
        jnp.ones((8, LANES), F32), squares, NT, precision=lax.Precision.HIGHEST, preferred_element_type=F32
    )
    for k in range(1, n_u):
        start(send(sq, sqx.at[k - 1], sq_sem, (k - 1,), t_to[k]))

    loads[1].wait()
    loads[2].wait()

    def low_step(i, acc):
        at_k = pl.ds(pl.multiple_of(i * kc, LANES), kc)
        left = jnp.concatenate([hs[rows_at(0, c, *half), at_k] for half in halves], axis=0)
        return acc + dot(bt[:, at_k], left, NT)

    low[...] = lax.fori_loop(0, depth // kc, low_step, jnp.zeros((rank, rows), F32))
    for k in range(1, n_u):
        start(send(low, lowx.at[k - 1], low_sem, (k - 1,), t_to[k]))

    def from_t(ref, extra, sems):
        total = ref[...]
        for k in range(1, n_u):
            send(ref, extra.at[k - 1], sems, (k - 1,), t_to[k]).wait_recv()
            total = total + extra[k - 1]
        return total

    square_sum = from_t(sq, sqx, sq_sem)
    mine = block_of(b, x, c)

    def packet(n, step):
        return [
            remote(a, pk_a.at[mine], pk_ssem.at[0, n], pk_rsem.at[0, n % n_blk], moved(step)),
            remote(pks, pk_s.at[mine], pk_ssem.at[1, n], pk_rsem.at[1, n % n_blk], moved(step)),
        ]

    @pl.when(u == t)
    def _():
        pks[...] = square_sum[0:1, :]
        pk_a[mine] = a[...]
        pk_s[mine] = square_sum[0:1, :]
        for n, step in enumerate(steps):
            if n:
                for copy in packet(n, step):
                    copy.start()

    for i in range(1, 3):
        start_h(i)
    for p in range(4, 8):
        start_wx(p)

    @pl.when(early)
    def _():
        for p in range(4, 8):
            start_wa(p)

    low_t = from_t(low, lowx, low_sem)
    low_tb = low_t.astype(BF16)
    low_b = jnp.transpose(low_t).astype(BF16)

    count = [0]
    waiting = [[], []]

    def lag_of(uu):
        return lax.rem(uu - t + 2 * n_u - 1, n_u)

    def lanes_in(j):
        first, size = chunks[j]
        return pl.ds(lane_at[j], padded(n_x * size))

    spans = {0: (0, 2 * rows), 1: (2 * rows, 2 * soon), 2: (0, 2 * (rows + soon))}

    def run_unit(kb, ku, j):
        first, size = chunks[j]
        wide = n_x * size
        top, tall = spans[kb]
        place = count[0] % 2
        count[0] += 1
        uu = shift(u, ku, n_u)
        keep = uu == t

        def copy():
            return remote(
                part_out.at[place, 0:tall, 0 : padded(wide)], part_in.at[lag_of(uu), top : top + tall, lanes_in(j)],
                ps_sem.at[place], pr_sem.at[min(kb, 1), j, lag_of(uu)], at(tensor=uu),
            )

        if waiting[place]:
            old_keep, old_copy = waiting[place].pop()

            @pl.when(jnp.logical_not(old_keep))
            def _():
                old_copy().wait_send()

        own[place, 0:tall, 0:wide] = jnp.zeros((tall, wide), F32)

        def unit_step(i, carry):
            at_k = pl.ds(pl.multiple_of(i * k_step, LANES), k_step)
            right = jnp.concatenate([ws[uu, xx, first : first + size, at_k] for xx in range(n_x)], axis=0)
            own[place, 0:tall, 0:wide] += dot(hs[top : top + tall, at_k], right, NT)
            return carry

        lax.fori_loop(0, depth // k_step, unit_step, 0)

        @pl.when(jnp.logical_not(keep))
        def _():
            part_out[place, 0:tall, 0:wide] = own[place, 0:tall, 0:wide].astype(BF16)
            copy().start()

        waiting[place].append((keep, copy))
        return kb, uu, j, place

    def scatter(kb, kc_, j):
        index = (kb * 2 + kc_, j)
        span = pl.ds(0, soon if kb else rows)
        return send(
            scat.at[kb * 2 + kc_, span, lanes_in(j)], got_out.at[far * 2 + c, span, lanes_in(j)], sc_sem, index,
            at(b=shift(b, kb, 2), core=shift(c, kc_, 2)),
        )

    def finish(kb, uu, j, place):
        first, size = chunks[j]
        wide = n_x * size
        top, tall = spans[kb]
        lanes = pl.ds(lane_at[j], wide)

        @pl.when(uu == t)
        def _():
            for k in range(n_u - 1):
                remote(
                    part_out.at[0, 0:tall, 0 : padded(wide)], part_in.at[k, top : top + tall, lanes_in(j)],
                    ps_sem.at[0], pr_sem.at[min(kb, 1), j, k], t_to[1],
                ).wait_recv()
            for side in (0, 1) if kb == 2 else (kb,):
                for kc_ in range(2):
                    for half in halves[: 1 if side else 2]:
                        at_c = row_of(side, shift(c, kc_, 2), half[0])
                        total = own[place, pl.ds(pl.multiple_of(at_c - top, 16), half[1]), 0:wide]
                        for k in range(n_u - 1):
                            more = part_in[k, pl.ds(pl.multiple_of(at_c, 16), half[1]), lanes]
                            total = total + more.astype(F32)
                        if side == 0 and kc_ == 0:
                            got_out[far * 2 + c, pl.ds(*half), lanes] = total.astype(BF16)
                        else:
                            scat[side * 2 + kc_, pl.ds(*half), lanes] = total.astype(BF16)
                    if side and deferred:
                        deferred[0].append((uu, side, kc_, j))
                    elif side or kc_:
                        scatter(side, kc_, j).start()

    pending, deferred = [], [[]]

    def go(kb, ku, j):
        new = run_unit(kb, ku, j)
        if pending:
            finish(*pending.pop())
        pending.append(new)

    def late_part(uu):
        return remote(late_out, late_in.at[lag_of(uu)], ls_sem.at[0], lr_sem.at[lag_of(uu)], at(tensor=uu))

    def late_unit(uu):
        late_sum[...] = jnp.zeros(late_sum.shape, F32)

        def late_step(i, carry):
            at_k = pl.ds(pl.multiple_of(i * k_step, LANES), k_step)
            right = jnp.concatenate(
                [ws[uu, xx, first : first + size, at_k] for first, size in chunks for xx in range(n_x)], axis=0
            )
            late_sum[...] += dot(right, hs[2 * (rows + soon) : 4 * rows, at_k], NT)
            return carry

        lax.fori_loop(0, depth // k_step, late_step, 0)
        flat = jnp.transpose(late_sum[...])
        return [(lane_at[j], flat[:, n_x * at : n_x * (at + size)]) for j, (at, size) in enumerate(chunks)]

    def late_scatter(kc_):
        return send(
            scat.at[2 + kc_, pl.ds(soon, late), :], got_out.at[far * 2 + c, pl.ds(soon, late), :], lsc_sem, (kc_,),
            at(b=1 - b, core=shift(c, kc_, 2)),
        )

    passed = [0]

    def pass_h():
        i = passed[0]
        passed[0] += 1
        got = h_rows(1, c, i)
        send(got, got, hb_sem, (i,), b_peer).wait_recv()
        start(send(got, got, hr_sem, (i,), core_peer))

    def near(p):
        for k in range(1, n_x):
            got = w_rows(u, shift(x, n_x - k, n_x), p)
            send(got, got, wx_sem, (k - 1, p), x_to[k]).wait_recv()

    def of_chunk(j):
        first, size = chunks[j]
        return [p for p in range(n_pc) if first <= pieces[p][0] < first + size]

    for q in range(n_blk):
        _, db, dx, dc = steps[q]
        src = block_of(shift(b, db, 2), shift(x, n_x - dx, n_x), shift(c, dc, 2))
        for wait in (
            remote(a, pk_a.at[src], pk_ssem.at[0, 0], pk_rsem.at[0, q], core_peer),
            remote(pks, pk_s.at[src], pk_ssem.at[1, 0], pk_rsem.at[1, q], core_peer),
        ):
            if q:
                wait.wait_recv()
            else:
                pl.when(u != t)(wait.wait_recv)

    mag_row = jnp.concatenate([mag[i : i + 1, :] for i in range(mag.shape[0])], axis=1)

    def scale_of(i, first, size):
        norm = jnp.sqrt(pk_s[i, 0:1, first : first + size] + 1e-06)
        return mag_row[:, i * cols + first : i * cols + first + size] / norm

    back_part = jnp.zeros((rank, rows), F32)
    for i in range(n_blk):
        piece = cot[:, i * cols : (i + 1) * cols].astype(F32)
        dpre = (piece * scale_of(i, 0, cols)).astype(BF16)
        back_part = back_part + dot(pk_a[i], dpre, NT)
        ga[i] = dot(low_tb, dpre, NN).astype(BF16)
    back[...] = back_part
    for k in range(1, n_u):
        start(send(back, backx.at[k - 1], back_sem, (k - 1,), t_to[k]))
    back_b = from_t(back, backx, back_sem).astype(BF16)
    backs[c] = back_b
    for k in range(1, 4):
        peer = at(b=shift(b, k // 2, 2), core=shift(c, k % 2, 2))
        start(send(backs.at[c], backs.at[k // 2 * 2 + c], tok_sem, (k - 1,), peer))

    for i in range(3, n_soon):
        start_h(i)
    for p in range(8, n_pc):
        start_wx(p)

    @pl.when(early)
    def _():
        for p in range(8, n_pc):
            start_wa(p)

    for i in range(2):
        send(half_rows(1 - c, i), half_rows(1 - c, i), hc_sem, (i,), core_peer).wait_recv()

    def turn(peer):
        pl.semaphore_signal(turn_sem, inc=1, device_id=peer, device_id_type=MESH)

    def w_arrived(k, p):
        got = w_rows(shift(u, n_u - k, n_u), x, p)
        send(got, got, wa_sem, (k - 1, p), u_to[k]).wait_recv()
        for m in range(1, n_x):
            send(got, got, wr_sem, (k - 1, m - 1, p), x_to[m]).start()

    for j in range(n_ch):
        while passed[0] < n_soon * (j + 1) // n_ch:
            pass_h()
        for p in of_chunk(j):
            near(p)
        if j >= n_ch - 2:

            @pl.when(early)
            def _():
                for k in range(1, n_u):
                    for p in range(n_pc):
                        if (p in of_chunk(n_ch - 1)) == (j == n_ch - 1):
                            w_arrived(k, p)
                if j == n_ch - 1:
                    turn(at(u=shift(u, 1, n_u)))

        if j == n_ch - 1:

            @pl.when(jnp.logical_not(early))
            def _():
                pl.semaphore_wait(turn_sem, 1)
                for p in range(n_pc):
                    start_wa(p)
                for i in range(n_soon, n_h):
                    late_h(i).start()

        go(0, 0, j)
    for i in range(n_soon):
        got = h_rows(1, 1 - c, i)
        send(got, got, hr_sem, (i,), core_peer).wait_recv()


    for k in range(1, 4):
        src = k // 2 * 2 + shift(c, k % 2, 2)
        send(backs.at[src], backs.at[src], tok_sem, (k - 1,), core_peer).wait_recv()

    def grad_of(kb, half, at_k):
        first, size = halves[half]
        total = jnp.zeros((rank, kc), F32)
        for cc in range(2):
            held = hs[row_of(kb, cc, first) : row_of(kb, cc, first) + size, at_k]
            total = total + dot(backs[kb * 2 + cc, :, first : first + size], held, NN)
        return total

    def grad_step(i, carry):
        at_k = pl.ds(pl.multiple_of(i * kc, LANES), kc)
        total = jnp.zeros((rank, kc), F32)
        for kb, half in ((0, 0), (0, 1), (1, 0)):
            total = total + grad_of(kb, half, at_k)
        gb[:, at_k] = total
        return carry

    lax.fori_loop(0, depth // kc, grad_step, 0)
    size_b = granule(depth, n_dp)
    share_b = depth // n_dp

    def lanes_of(device):
        return pl.ds(pl.multiple_of(lax.div(place_of(device) * share_b, size_b) * size_b, LANES), size_b)

    groups = [step for step in steps if step[1] == 0 and step[3] == 0]
    def emit(bb, cc, j, half):
        first, size = chunks[j]
        span = pl.ds(*halves[half])
        for xx in range(n_x):
            i = block_of(bb, xx, cc)
            left = i * cols + first
            lane = lane_at[j] + xx * size
            pre = got_out[bb * 2 + cc, span, lane : lane + size].astype(F32)
            low_half = low_b[halves[half][0] : sum(halves[half]), :]
            pre = pre + dot(low_half, pk_a[i, :, first : first + size], NN)
            mixed[span, left : left + size] = (pre * scale_of(i, first, size)).astype(BF16)
            part = jnp.sum(cot[span, left : left + size].astype(F32) * pre, axis=0, keepdims=True)
            if half:
                mg[i, 0:1, first : first + size] += part
            else:
                mg[i, 0:1, first : first + size] = part

    def scattered(bb, cc, j, span):
        kind = lax.rem(bb + far, 2) * 2 + lax.rem(cc + c, 2)
        got = got_out.at[bb * 2 + cc, span, lanes_in(j)]
        return send(got, got, sc_sem, (kind, j), core_peer)

    def near_outputs(which):
        for bb in range(2):

            @pl.when(bb == far)
            def _():
                for j in which:
                    for cc in range(2):
                        pl.when(cc != c)(scattered(bb, cc, j, pl.ds(0, rows)).wait_recv)
                        for half in range(2):
                            emit(bb, cc, j, half)

    def far_outputs(which, half):
        for bb in range(2):

            @pl.when(bb != far)
            def _():
                for j in which:
                    for cc in range(2):
                        if half == 0:
                            scattered(bb, cc, j, pl.ds(0, soon)).wait_recv()
                        emit(bb, cc, j, half)

    def far_piece(k, p):
        @pl.when(jnp.logical_not(early))
        def _():
            w_arrived(k, p)
            if k == n_u - 1 and p == n_pc - 1:
                turn(b_peer)

    def far_ready(k, j):
        for p in of_chunk(j):
            for m in range(1, n_x):
                got = w_rows(shift(u, n_u - k, n_u), shift(x, n_x - m, n_x), p)
                send(got, got, wr_sem, (k - 1, m - 1, p), x_to[m]).wait_recv()

    units = [(1, 0, j) for j in range(n_ch)]
    early_out = 2 if n_ch > 2 else 0

    for k in range(1, n_u):
        for p in range(n_pc):
            if pending:
                finish(*pending.pop())
            elif units:
                pending.append(run_unit(*units.pop(0)))
            if k == n_u - 1 and n_ch > 2 and p == n_pc - 5:
                near_outputs([0])
            far_piece(k, p)
            for j in range(n_ch - 1):
                if max(of_chunk(j)) + 2 == p:
                    far_ready(k, j)
                    units += [(0, n_u - k, j), (1, n_u - k, j)]
        if k == n_u - 1:

            @pl.when(early)
            def _():
                pl.semaphore_wait(turn_sem, 1)
                late_h(n_soon).start()

        while units:
            go(*units.pop(0))
        if k == n_u - 1:
            near_outputs(range(max(early_out - 1, 0), early_out))
        for j in range(n_ch):
            if max(of_chunk(j)) + 2 >= n_pc:
                far_ready(k, j)
                if k == n_u - 1 and deferred:
                    for uu, side, kc_, i in deferred.pop():
                        pl.when(uu == t)(scatter(side, kc_, i).start)
                go(2, n_u - k, j)

    for i in range(n_soon, n_h):
        pass_h()
    for i in range(n_soon, n_h):
        got = h_rows(1, 1 - c, i)
        send(got, got, hr_sem, (i,), core_peer).wait_recv()
    for k in range(1, n_u):
        if k > 1:
            late_part(shift(t, k - 1, n_u)).wait_send()
        for lane, part in late_unit(shift(t, k, n_u)):
            late_out[:, lane : lane + part.shape[1]] = part.astype(BF16)
        late_part(shift(t, k, n_u)).start()
    finish(*pending.pop())

    def grad_late(i, carry):
        at_k = pl.ds(pl.multiple_of(i * kc, LANES), kc)
        gb[:, at_k] += grad_of(1, 1, at_k)
        return carry

    lax.fori_loop(0, depth // kc, grad_late, 0)
    for n, step in enumerate(groups):
        if n:
            peer = moved(step)
            start(send(gb.at[:, lanes_of(peer)], gbx.at[n], gb_sem, (n,), peer))
    for lane, part in late_unit(t):
        late_own[:, lane : lane + part.shape[1]] = part

    for k in range(n_u - 1):
        remote(late_out, late_in.at[k], ls_sem.at[0], lr_sem.at[k], t_to[1]).wait_recv()
    for kc_ in range(2):
        at_c = pl.ds(pl.multiple_of(shift(c, kc_, 2) * late, 16), late)
        for j, (_, size) in enumerate(chunks):
            lanes = pl.ds(lane_at[j], n_x * size)
            total = late_own[at_c, lanes]
            for k in range(n_u - 1):
                total = total + late_in[k, at_c, lanes].astype(F32)
            scat[2 + kc_, pl.ds(soon, late), lanes] = total.astype(BF16)
        late_scatter(kc_).start()
    for n, step in enumerate(steps):
        if n:
            peer = moved(step)
            start(send(ga.at[lax.div(place_of(peer), n_u)], gax.at[n], ga_sem, (n,), peer))
    near_outputs(range(early_out, n_ch))
    far_outputs(range(n_ch), 0)
    for kc_ in range(2):
        got = got_out.at[(1 - far) * 2 + shift(c, kc_, 2), pl.ds(soon, late), :]
        send(got, got, lsc_sem, (kc_,), core_peer).wait_recv()
    far_outputs(range(n_ch), 1)

    for n, step in enumerate(steps):
        if n:
            peer = moved(step)
            start(send(mg.at[lax.div(place_of(peer), n_u)], mgx.at[n], mg_sem, (n,), peer))

    block = lax.div(place_of(at()), n_u)
    total = ga[block].astype(F32)
    for n in range(1, n_dp):
        send(ga.at[0], gax.at[n], ga_sem, (n,), core_peer).wait_recv()
        total = total + gax[n].astype(F32)
    share = cols // n_u
    for q in range(n_u):

        @pl.when(lax.rem(place_of(at()), n_u) == q)
        def _():
            ga_out[...] = total[:, q * share : (q + 1) * share]

    total = gb[:, lanes_of(at())]
    for n in range(1, len(groups)):
        send(gbx.at[0], gbx.at[n], gb_sem, (n,), core_peer).wait_recv()
        total = total + gbx[n]
    for q in range(size_b // share_b):

        @pl.when(lax.rem(place_of(at()), size_b // share_b) == q)
        def _():
            gb_out[...] = total[:, q * share_b : (q + 1) * share_b]

    for place in range(2):
        for keep, copy in waiting[place]:

            @pl.when(jnp.logical_not(keep))
            def _():
                copy().wait_send()

    @pl.when(u == t)
    def _():
        for n, step in enumerate(steps):
            if n:
                for copy in packet(n, step):
                    copy.wait_send()

    for k in range(1, n_u):
        for p in range(n_pc):
            wa(k, p).wait_send()
            got = w_rows(shift(u, n_u - k, n_u), x, p)
            for m in range(1, n_x):
                send(got, got, wr_sem, (k - 1, m - 1, p), x_to[m]).wait_send()
    for i in range(n_soon, n_h):
        late_h(i).wait_send()
    late_part(shift(t, n_u - 1, n_u)).wait_send()
    for kc_ in range(2):
        late_scatter(kc_).wait_send()
    for kb in range(2):
        for kc_ in range(2):
            if kb or kc_:
                for j in range(n_ch):
                    scatter(kb, kc_, j).wait_send()
    for copy in sent:
        copy.wait_send()

    total = mg[block]
    for n in range(1, n_dp):
        send(mg.at[0], mgx.at[n], mg_sem, (n,), core_peer).wait_recv()
        total = total + mgx[n]
    total = total / jnp.sqrt(pk_s[block] + 1e-06)
    for q in range(n_u):

        @pl.when(lax.rem(place_of(at()), n_u) == q)
        def _():
            mag_out[...] = total[:, q * share : (q + 1) * share]


def fused(hidden, weight_t, factor_bt, factor_a, magnitude, cotangent, n_u, n_x):
    rows, depth = hidden.shape
    cols = weight_t.shape[0]
    rank = factor_a.shape[0]
    n_blk = 4 * n_x
    n_dp = n_blk * n_u
    n_ch, n_pc = len(chunks_of(cols, n_x)), len(cuts(cols, PIECE))
    wide = n_x * LANES
    full = sum(padded(n_x * size) for _, size in chunks_of(cols, n_x))
    late = rows // LATE_SHARE
    n_h = len(cuts(rows - late, H_PIECE)) + 1
    size_b = granule(depth, n_dp)
    groups = n_u * n_x
    few = max(n_x - 1, 1)
    sem = pltpu.SemaphoreType.DMA
    vmem = pltpu.VMEM
    whole = pl.BlockSpec(memory_space=pltpu.VMEM)
    return pl.pallas_call(
        functools.partial(kernel, n_u, n_x),
        out_shape=(
            jax.ShapeDtypeStruct(cotangent.shape, BF16),
            jax.ShapeDtypeStruct((1, cols // n_u), F32),
            jax.ShapeDtypeStruct((rank, cols // n_u), F32),
            jax.ShapeDtypeStruct((rank, depth // n_dp), F32),
        ),
        in_specs=[pl.BlockSpec(memory_space=pltpu.HBM)] * 2 + [whole] * 4,
        out_specs=(whole,) * 4,
        scratch_shapes=[
            vmem((4 * rows, depth), BF16),
            vmem((n_u, n_x, cols, depth), BF16),
            vmem((2, 4 * rows - 2 * late, wide), F32),
            vmem((2, 4 * rows - 2 * late, wide), BF16),
            vmem((n_u - 1, 4 * rows - 2 * late, full), BF16),
            vmem((4, rows, full), BF16),
            vmem((n_x * cols, 2 * late), F32),
            vmem((2 * late, full), F32),
            vmem((2 * late, full), BF16),
            vmem((n_u - 1, 2 * late, full), BF16),
            vmem((4, rows, full), BF16),
            vmem((8, cols), F32),
            vmem((n_u - 1, 8, cols), F32),
            vmem((rank, rows), F32),
            vmem((n_u - 1, rank, rows), F32),
            vmem((rank, rows), F32),
            vmem((n_u - 1, rank, rows), F32),
            vmem((4, rank, rows), BF16),
            vmem((n_blk, rank, cols), BF16),
            vmem((n_blk, 1, cols), F32),
            vmem((1, cols), F32),
            vmem((n_blk, rank, cols), BF16),
            vmem((n_dp, rank, cols), BF16),
            vmem((rank, depth), F32),
            vmem((groups, rank, size_b), F32),
            vmem((n_blk, 1, cols), F32),
            vmem((n_dp, 1, cols), F32),
            sem((3,)),
            sem((2, 2)),
            sem((2, n_h)),
            sem((2, n_h)),
            sem((2, few, n_pc)),
            sem((2, n_u - 1, n_pc)),
            sem((2, n_u - 1, few, n_pc)),
            sem((2,)),
            sem((2, n_ch, n_u - 1)),
            sem((2, 4, n_ch)),
            sem((1,)),
            sem((n_u - 1,)),
            sem((2, 2)),
            pltpu.SemaphoreType.REGULAR,
            sem((2, n_u - 1)),
            sem((2, n_u - 1)),
            sem((2, n_u - 1)),
            sem((2, 3)),
            sem((2, n_dp)),
            sem((2, n_blk)),
            sem((2, n_dp)),
            sem((2, groups)),
            sem((2, n_dp)),
        ],
        compiler_params=pltpu.CompilerParams(
            collective_id=0, has_side_effects=True, vmem_limit_bytes=67043328
        ),
        name="fused",
    )(hidden, weight_t, factor_bt, factor_a, magnitude, cotangent)


def in_rows(values):
    return values.reshape(-1, LANES) if values.shape[0] % LANES == 0 else values[None]


def body(hidden, weight, factor_b, factor_a, magnitude, cotangent, *, n_u, n_x):
    mixed, mag, ga, gb = fused(
        hidden, weight.T, factor_b.T, factor_a, in_rows(magnitude), cotangent, n_u, n_x
    )
    return mixed, mag[0], ga, gb.T


def solution(mesh):
    n_dp, n_u = mesh.shape["dp"], mesh.shape["tensor"]
    n_x = n_dp // (4 * n_u)
    fine = Mesh(mesh.devices.reshape(n_u, 2, n_x, 2, n_u), AXES)
    dp = ("u", "b", "x", "core")

    def step(*args):
        return body(*args, n_u=n_u, n_x=n_x)

    return jax.shard_map(
        step,
        mesh=fine,
        in_specs=(
            P(dp, "tensor"),
            P("tensor", dp),
            P("tensor", None),
            P(None, dp),
            P("tensor"),
            P(dp, "tensor"),
        ),
        out_specs=(
            P(dp, "tensor"),
            P(("tensor",) + dp),
            P(None, ("tensor",) + dp),
            P(("tensor",) + dp, None),
        ),
        check_vma=False,
    )
```
